128 devices in a mesh: row: 16 (over y, x_lo, core), col: 8 (over x_hi, z).
Axes of the slice: x: 4 (x_hi: 2, x_lo: 2; x = x_hi * 2 + x_lo), y: 4, z: 4, core: 2. Of those that a mesh axis runs over, the one named last changes fastest.
Arguments:
- lower_inverse: float32 [16, 8, 1024, 1024], P('row', 'col'), may hold values from -1 to 2, as said below
- upper_inverse: float32 [16, 8, 1024, 1024], P('row', 'col'), may hold values from -1 to 2, as said below
- left_coupling: bfloat16 [16, 8, 512, 1024], P('row', 'col'), may hold values from -0.1875 to 0.1875
- right_pieces: float32 [8, 1024, 2048], P('col', None, 'row'), may hold values from -6 to 6
- interface_block: int32 [16, 8, 4], P('row', 'col'), may hold values from 0 to 7, all different within a row
- a_gg: float32 [16, 1024, 2048], P('row', 'col'), may hold values from -6 to 6
- panel_order: int32 [16], replicated, may hold values from 0 to 15, each once
Outputs:
- schur: float32 [16, 1024, 2048], P('row', 'col')
The draws below stay inside these ranges and needn't reach their ends.
Inputs may be any that keep to these rules, and one draw needn't show every extreme that they name: `interface_block`: the 4 block ids of one subdomain are distinct. `panel_order`: A permutation of the column blocks. `lower_inverse`: lower triangular, diagonal between 1 and 2. `upper_inverse`: upper triangular, diagonal between 1 and 2.
All inputs are finite; a program needn't handle non-finite values.
Results may differ from the reference program's by a relative error of at most 0.0028.
Values sent between devices are 32-bit elements; how exact they have to be, the bound alone decides.
A program may use at most 128 MiB of HBM per device.

```python
import jax
import jax.numpy as jnp
from jax import lax

NI = 1024
PW = 2048
WB = 128
KB = 4
PR = 1024
N_ROW = 16
N_COL = 8


def make_factor(key, below):
    first_key, second_key = jax.random.split(key)
    shape = (N_ROW, N_COL, NI, NI)
    spread = jnp.clip(jax.random.normal(first_key, shape, jnp.float32), -6.0, 6.0) * (0.5 / NI ** 0.5)
    diagonal = jax.random.uniform(second_key, (N_ROW, N_COL, NI), jnp.float32, 1.0, 2.0)
    rows = lax.broadcasted_iota(jnp.int32, (NI, NI), 0)
    cols = lax.broadcasted_iota(jnp.int32, (NI, NI), 1)
    if below:
        keep = rows > cols
    else:
        keep = rows < cols
    ones = (rows == cols).astype(jnp.float32)
    return jnp.where(keep, spread, 0.0) + diagonal[..., None] * ones


def draw_lower_inverse(key, part):
    return make_factor(jax.random.fold_in(key, 11), True)


def draw_upper_inverse(key, part):
    return make_factor(jax.random.fold_in(key, 23), False)


def steps_of(stream_key, shape, cuts, least, top_value):
    def one(dim, shards_of):
        steps = jax.random.uniform(jax.random.fold_in(jax.random.fold_in(stream_key, 6), dim), (shards_of,), jnp.float32, least / len(cuts), top_value / len(cuts))
        return jnp.repeat(jnp.exp(steps), shape[dim] // shards_of).reshape((-1,) + (1,) * (len(shape) - dim - 1))

    loudness = one(*cuts[0])
    for cut in cuts[1:]:
        loudness = loudness * one(*cut)
    return loudness


def different_ones(own_key, rows, number_of, top, lift):
    sequence = jax.random.permutation(jax.random.fold_in(own_key, 1), number_of)
    boost = sequence
    for power in range(3):
        boost = boost * boost // number_of
    boost = boost * lift // number_of
    tickets = jax.random.randint(jax.random.fold_in(own_key, 2), (rows, number_of), 0, 4096) + boost
    holders = jax.random.permutation(jax.random.fold_in(own_key, 3), rows)[jnp.arange(number_of) % rows]
    tickets = jnp.where(jnp.arange(rows)[:, None] == holders[None, :], 1 << 14, tickets)
    priority = tickets * number_of + jnp.arange(number_of)
    return lax.top_k(priority.astype(jnp.int32), top)[1].astype(jnp.int32)


def noise(stream_key, shape, scale, bound, cuts=(), held_as=jnp.bfloat16):
    array = scale * jax.random.normal(stream_key, shape, jnp.float32)
    if cuts:
        array = array * steps_of(stream_key, shape, cuts, -0.22, 0.18)
    return jnp.clip(array, -bound, bound).astype(held_as)


def setup_inputs(seed: int = 0) -> dict:
    streams_of = jax.random.split(jax.random.key(seed), 8)
    lower_inverse = draw_lower_inverse(jax.random.fold_in(streams_of[7], 71), 0)
    upper_inverse = draw_upper_inverse(jax.random.fold_in(streams_of[7], 71), 0)
    left_coupling = noise(streams_of[2], (N_ROW, N_COL, KB * WB, NI), NI ** -0.5, 0.1875, ((0, 16), (1, 8)))
    right_pieces = noise(streams_of[3], (N_COL, NI, PW), 1.0, 6.0, ((0, 8), (2, 16)), jnp.float32)
    interface_block = different_ones(streams_of[4], N_ROW * N_COL, N_COL, KB, 0).reshape((N_ROW, N_COL, KB))
    a_gg = noise(streams_of[5], (N_ROW, PR, PW), 1.0, 6.0, ((0, 16), (1, 8)), jnp.float32)
    panel_order = jax.random.permutation(streams_of[6], N_ROW).astype(jnp.int32)
    return {"lower_inverse": lower_inverse, "upper_inverse": upper_inverse, "left_coupling": left_coupling, "right_pieces": right_pieces, "interface_block": interface_block, "a_gg": a_gg, "panel_order": panel_order}


def column_order(panel_order):
    length = panel_order.shape[0]
    positions = jnp.arange(length, dtype=jnp.int32)
    hits = (panel_order[:, None] == positions[None, :]).astype(jnp.int32)
    return jnp.sum(hits * positions[:, None], axis=0).astype(jnp.int32)


def couple(lower_mat, upper_mat, left_mat, panel):
    halfway = jnp.dot(lower_mat, panel, precision=lax.Precision.HIGHEST, preferred_element_type=jnp.float32)
    solved = jnp.dot(upper_mat, halfway, precision=lax.Precision.HIGHEST, preferred_element_type=jnp.float32)
    solved = solved.astype(jnp.bfloat16)
    return jnp.dot(left_mat, solved, preferred_element_type=jnp.float32)


def place_rows(coupled, block_ids, first_block, block_total):
    block_count = block_ids.shape[0]
    block_rows = coupled.shape[0] // block_count
    targets = first_block + jnp.arange(block_total, dtype=jnp.int32)
    placed = (block_ids[:, None] == targets[None, :]).astype(jnp.float32)
    shaped = coupled.reshape(block_count, block_rows, coupled.shape[1])
    spread = jnp.einsum("kb,kwp->bwp", placed, shaped, precision=lax.Precision.HIGHEST)
    return spread.reshape(block_total * block_rows, coupled.shape[1])


def reference(lower_inverse, upper_inverse, left_coupling, right_pieces, interface_block, a_gg, panel_order):
    row_count = lower_inverse.shape[0]
    col_count = lower_inverse.shape[1]
    inner = right_pieces.shape[1]
    width_piece = right_pieces.shape[2] // row_count
    order = column_order(panel_order)
    panels = right_pieces.reshape(col_count, inner, row_count, width_piece)[:, :, order, :]
    panels = panels.reshape(col_count, inner, row_count * width_piece)

    def one_row(row_args):
        lowers, uppers, lefts, blocks, base = row_args

        def add_one(summed, item):
            lower_mat, upper_mat, left_mat, block_ids, panel = item
            coupled = couple(lower_mat, upper_mat, left_mat, panel)
            return summed + place_rows(coupled, block_ids, 0, col_count), None

        summed, _ = lax.scan(add_one, jnp.zeros(base.shape, jnp.float32), (lowers, uppers, lefts, blocks, panels))
        return base - summed

    return lax.map(one_row, (lower_inverse, upper_inverse, left_coupling, interface_block, a_gg))
```

```python
import functools

import jax
import jax.numpy as jnp
from jax import lax
from jax.experimental import pallas as pl
from jax.experimental.pallas import tpu as pltpu
from jax.sharding import PartitionSpec as P

MESH = pl.DeviceIdType.MESH
F32, BF16 = jnp.float32, jnp.bfloat16

NI = 1024
WB = 128
CW = 2 * WB
NCH = 8
TB = 256

UP, DN = 48, 40
XU, XD = 16, 24
RA = UP + DN
XR = XU + XD
A_UP, A_DN, A_ALL = pl.ds(0, UP), pl.ds(UP, DN), pl.ds(0, RA)
X_UP, X_DN, X_ALL = pl.ds(RA, XU), pl.ds(RA + XU, XD), pl.ds(RA, XR)

CHUNKS = ((0, 0), (3, 0), (1, 0), (0, 1), (3, 1), (1, 1), (2, 0), (2, 1))


def coords():
    r, c = lax.axis_index("row"), lax.axis_index("col")
    return r // 4, (r // 2) % 2, r % 2, c // 4, c % 4


def device(y, xl, core, xh, z):
    return (y * 4 + xl * 2 + core, xh * 4 + z)


def split(x):
    hi = x.astype(BF16)
    return hi, (x - hi.astype(F32)).astype(BF16)


def main_kernel(
    ids, low_hbm, upp_hbm, left_hbm, piece_hbm, out,
    low32, upp32, left_v, panel, low_hi, low_lo, upp_hi, upp_lo, left_d,
    p_hi, p_lo, h_hi, h_lo, solved, part,
    rp2, rq2, fp, fq, fpa, fqa, fx2, rx, rxp2, rxq2, fxp, fxq, fxpa, fxqa,
    loc_sem, ag_s, ag_r, par_s, par_r, rs_s, rs_r,
):
    y, xl, core, xh, z = coords()
    partner = device(y, xl, 1 - core, xh, z)
    across = device(y, 1 - xl, core, xh, z)
    yp = device((y + 1) % 4, xl, core, xh, z)
    ym = device((y + 3) % 4, xl, core, xh, z)
    zp = device(y, xl, core, xh, (z + 1) % 4)
    zm = device(y, xl, core, xh, (z + 3) % 4)
    far = device(y, xl, core, 1 - xh, z)

    own = pltpu.make_async_copy(piece_hbm, panel.at[0, 0], loc_sem.at[0])
    own.start()
    loads = []
    for b in range(4):
        rows = pl.ds(b * TB, TB)
        cols = pl.ds(0, (b + 1) * TB)
        loads.append(pltpu.make_async_copy(low_hbm.at[rows, cols], low32.at[rows, cols], loc_sem.at[1 + b]))
    for b in range(4):
        rows = pl.ds(b * TB, TB)
        cols = pl.ds(b * TB, NI - b * TB)
        loads.append(pltpu.make_async_copy(upp_hbm.at[rows, cols], upp32.at[rows, cols], loc_sem.at[5 + b]))
    left_load = pltpu.make_async_copy(left_hbm, left_v, loc_sem.at[9])
    for copy in loads:
        copy.start()
    left_load.start()

    barrier = pltpu.get_barrier_semaphore()
    for peer in (partner, across, yp, ym, zp, zm, far):
        pl.semaphore_signal(barrier, inc=1, device_id=peer, device_id_type=MESH)
    pl.semaphore_wait(barrier, 7)

    def link(n, src, dst, peer):
        return pltpu.make_async_remote_copy(
            src_ref=panel.at[src, 0], dst_ref=panel.at[dst, 0], send_sem=ag_s.at[n],
            recv_sem=ag_r.at[dst], device_id=peer, device_id_type=MESH)

    links = (
        link(0, 0, 1, yp), link(1, 0, 2, ym), link(2, 0, 3, across),
        link(3, 3, 4, yp), link(4, 3, 5, ym), link(5, 1, 6, yp), link(6, 5, 7, ym))
    landing = {1: links[0], 2: links[1], 3: links[2], 4: links[3], 5: links[4], 6: links[5], 7: links[6]}

    def share(i):
        return pltpu.make_async_remote_copy(
            src_ref=panel.at[i, 0], dst_ref=panel.at[i, 1], send_sem=par_s.at[i],
            recv_sem=par_r.at[i], device_id=partner, device_id_type=MESH)

    own.wait()
    share(0).start()
    for n in (0, 1, 2):
        links[n].start()

    strip = 32
    for b in range(4):
        loads[b].wait()

        @pl.loop(0, TB // strip)
        def _(s, b=b):
            rows = pl.ds(pl.multiple_of(b * TB + s * strip, strip), strip)
            cols = pl.ds(0, (b + 1) * TB)
            low_hi[rows, cols], low_lo[rows, cols] = split(low32[rows, cols])
    for b in range(4):
        loads[4 + b].wait()

        @pl.loop(0, TB // strip)
        def _(s, b=b):
            rows = pl.ds(pl.multiple_of(b * TB + s * strip, strip), strip)
            cols = pl.ds(b * TB, NI - b * TB)
            upp_hi[rows, cols], upp_lo[rows, cols] = split(upp32[rows, cols])

    left_load.wait()
    for dx in range(2):
        for dz in range(4):
            block = ((xh + dx) % 2) * 4 + (z + dz) % 4
            place = jnp.int32(0)
            touched = jnp.int32(0)
            for k in range(4):
                hit = ids[k] == block
                place = jnp.where(hit, k, place)
                touched = jnp.where(hit, 1, touched)
            left_d[dx, dz] = jnp.where(touched > 0, left_v[place], jnp.zeros((WB, NI), BF16))

    def reduce_copies(i):
        def send(n, src, dst, peer):
            return pltpu.make_async_remote_copy(
                src_ref=src, dst_ref=dst.at[i], send_sem=rs_s.at[i, n], recv_sem=rs_r.at[i, n],
                device_id=peer, device_id_type=MESH)

        both = slice(None)
        return (
            send(0, part.at[i, both, 2, A_UP], rp2, zp),
            send(1, part.at[i, both, 2, A_DN], rq2, zm),
            send(2, part.at[i, both, 1, A_DN], fq, zp),
            send(3, part.at[i, both, 3, A_UP], fp, zm),
            send(4, part.at[i, 1, both, X_ALL], rx, far),
            send(5, part.at[i, both, 1, A_UP], fpa, zp),
            send(6, part.at[i, both, 3, A_DN], fqa, zm),
            send(7, part.at[i, 0, 2, X_UP], rxp2, zp),
            send(8, part.at[i, 0, 2, X_DN], rxq2, zm),
            send(9, part.at[i, 0, 1, X_DN], fxq, zp),
            send(10, part.at[i, 0, 3, X_UP], fxp, zm),
            send(11, part.at[i, 1, 0, A_ALL], fx2, far),
            send(12, part.at[i, 0, 1, X_UP], fxpa, zp),
            send(13, part.at[i, 0, 3, X_DN], fxqa, zm),
        )

    def multiply(i):
        for h in range(2):
            @pl.loop(0, 8)
            def _(s, h=h):
                rows = pl.ds(pl.multiple_of(s * WB, WB), WB)
                cols = pl.ds(h * WB, WB)
                p_hi[rows, cols], p_lo[rows, cols] = split(panel[i, h, rows, :])

        def dot(a, b):
            return jnp.dot(a, b, preferred_element_type=F32)

        for b in range(4):
            rows, cols = pl.ds(b * TB, TB), pl.ds(0, (b + 1) * TB)
            a_hi = low_hi[rows, cols]
            half = dot(a_hi, p_hi[cols]) + dot(a_hi, p_lo[cols]) + dot(low_lo[rows, cols], p_hi[cols])
            h_hi[rows, :], h_lo[rows, :] = split(half)
        for b in range(4):
            rows, cols = pl.ds(b * TB, TB), pl.ds(b * TB, NI - b * TB)
            a_hi = upp_hi[rows, cols]
            full = dot(a_hi, h_hi[cols]) + dot(a_hi, h_lo[cols]) + dot(upp_lo[rows, cols], h_hi[cols])
            solved[rows, :] = full.astype(BF16)
        for dx in range(2):
            for dz in range(4):
                part[i, dx, dz] = dot(left_d[dx, dz], solved[...])

    @pl.loop(0, NCH + 3)
    def _(step):
        for at, arrivals in ((1, (1, 3, 2)), (3, (4, 5)), (5, (6, 7))):
            @pl.when(step == at)
            def _(arrivals=arrivals):
                for a in arrivals:
                    landing[a].wait_recv()
                    for n in {1: (5,), 3: (3, 4), 5: (6,)}.get(a, ()):
                        links[n].start()
                    share(a).start()

        @pl.when(step < NCH)
        def _():
            share(step).wait_recv()
            multiply(step)
            copies = reduce_copies(step)
            for n in range(5):
                copies[n].start()

        @pl.when((step >= 1) & (step < NCH + 1))
        def _():
            i = step - 1
            copies = reduce_copies(i)
            copies[0].wait_recv()
            part[i, :, 1, A_UP] += rp2[i]
            copies[5].start()
            copies[1].wait_recv()
            part[i, :, 3, A_DN] += rq2[i]
            copies[6].start()
            copies[4].wait_recv()
            part[i, 0, :, X_ALL] += rx[i]
            for n in (7, 8, 9, 10):
                copies[n].start()

        @pl.when((step >= 2) & (step < NCH + 2))
        def _():
            i = step - 2
            copies = reduce_copies(i)
            for n in (2, 3, 5, 6):
                copies[n].wait_recv()
            part[i, :, 0, A_UP] += fp[i] + fpa[i]
            part[i, :, 0, A_DN] += fq[i] + fqa[i]
            copies[11].start()
            copies[7].wait_recv()
            part[i, 0, 1, X_UP] += rxp2[i]
            copies[12].start()
            copies[8].wait_recv()
            part[i, 0, 3, X_DN] += rxq2[i]
            copies[13].start()

        @pl.when(step >= 3)
        def _():
            i = step - 3
            copies = reduce_copies(i)
            for n in (9, 10, 11, 12, 13):
                copies[n].wait_recv()
            out[i, A_ALL] = part[i, 0, 0, A_ALL] + fx2[i]
            out[i, X_UP] = part[i, 0, 0, X_UP] + (fxp[i] + fxpa[i])
            out[i, X_DN] = part[i, 0, 0, X_DN] + (fxq[i] + fxqa[i])

    for copy in links:
        copy.wait_send()

    @pl.loop(0, NCH)
    def _(i):
        share(i).wait_send()
        for copy in reduce_copies(i):
            copy.wait_send()


def place_kernel(order, owned, base, out):
    y, xl, core, _, _ = coords()
    for j, (dy, dx) in enumerate(CHUNKS):
        for h in range(2):
            source = ((y + dy) % 4) * 4 + ((xl + dx) % 2) * 2 + (core + h) % 2
            cols = pl.ds(pl.multiple_of(order[source] * WB, WB), WB)
            out[:, cols] = base[:, cols] - owned[j, :, h * WB:(h + 1) * WB]


def per_device(lower_inverse, upper_inverse, left_coupling, right_pieces, interface_block, a_gg, panel_order):
    vmem = pl.BlockSpec(memory_space=pltpu.VMEM)
    smem = pl.BlockSpec(memory_space=pltpu.SMEM)
    hbm = pl.BlockSpec(memory_space=pltpu.HBM)

    def buf(*shape, dtype=F32):
        return pltpu.VMEM(shape, dtype)

    dma = pltpu.SemaphoreType.DMA
    owned = pl.pallas_call(
        main_kernel,
        name="assemble",
        out_shape=jax.ShapeDtypeStruct((NCH, WB, CW), F32),
        in_specs=[smem, hbm, hbm, hbm, hbm],
        out_specs=vmem,
        scratch_shapes=[
            buf(NI, NI), buf(NI, NI), buf(4, WB, NI, dtype=BF16), buf(NCH, 2, NI, WB),
            buf(NI, NI, dtype=BF16), buf(NI, NI, dtype=BF16), buf(NI, NI, dtype=BF16), buf(NI, NI, dtype=BF16),
            buf(2, 4, WB, NI, dtype=BF16),
            buf(NI, CW, dtype=BF16), buf(NI, CW, dtype=BF16), buf(NI, CW, dtype=BF16), buf(NI, CW, dtype=BF16),
            buf(NI, CW, dtype=BF16), buf(NCH, 2, 4, WB, CW),
            buf(NCH, 2, UP, CW), buf(NCH, 2, DN, CW), buf(NCH, 2, UP, CW), buf(NCH, 2, DN, CW),
            buf(NCH, 2, UP, CW), buf(NCH, 2, DN, CW), buf(NCH, RA, CW),
            buf(NCH, 4, XR, CW), buf(NCH, XU, CW), buf(NCH, XD, CW), buf(NCH, XU, CW), buf(NCH, XD, CW),
            buf(NCH, XU, CW), buf(NCH, XD, CW),
            dma((10,)), dma((7,)), dma((NCH,)), dma((NCH,)), dma((NCH,)), dma((NCH, 14)), dma((NCH, 14)),
        ],
        compiler_params=pltpu.CompilerParams(
            collective_id=0, has_side_effects=True, vmem_limit_bytes=60 * 2**20),
    )(
        interface_block[0, 0], lower_inverse[0, 0], upper_inverse[0, 0],
        left_coupling[0, 0].reshape(4, WB, NI), right_pieces[0])
    schur = pl.pallas_call(
        place_kernel,
        name="place",
        out_shape=jax.ShapeDtypeStruct(a_gg.shape[1:], F32),
        in_specs=[smem, vmem, vmem],
        out_specs=vmem,
    )(panel_order, owned, a_gg[0])
    return schur[None]


def solution(mesh):
    return jax.shard_map(
        per_device,
        mesh=mesh,
        in_specs=(
            P("row", "col", None, None),
            P("row", "col", None, None),
            P("row", "col", None, None),
            P("col", None, "row"),
            P("row", "col", None),
            P("row", "col", None),
            P(),
        ),
        out_specs=P("row", "col", None),
        check_vma=False,
    )
```

```python
import functools

import jax
import jax.numpy as jnp
from jax import lax
from jax.experimental import pallas as pl
from jax.experimental.pallas import tpu as pltpu
from jax.sharding import PartitionSpec as P

MESH = pl.DeviceIdType.MESH
F32, BF16 = jnp.float32, jnp.bfloat16

NI = 1024
WB = 128
CW = 2 * WB
NCH = 8
TB = 256

UP, DN = 48, 40
XU, XD = 16, 24
RA = UP + DN
XR = XU + XD
A_UP, A_DN, A_ALL = pl.ds(0, UP), pl.ds(UP, DN), pl.ds(0, RA)
X_UP, X_DN, X_ALL = pl.ds(RA, XU), pl.ds(RA + XU, XD), pl.ds(RA, XR)

CHUNKS = ((0, 0), (-1, 0), (1, 0), (0, 1), (2, 0), (-1, 1), (1, 1), (2, 1))


def coords():
    r, c = lax.axis_index("row"), lax.axis_index("col")
    return r // 4, (r // 2) % 2, r % 2, c // 4, c % 4


def device(y, xl, core, xh, z):
    return (y * 4 + xl * 2 + core, xh * 4 + z)


def split(x):
    hi = x.astype(BF16)
    return hi, (x - hi.astype(F32)).astype(BF16)


def main_kernel(
    ids, low_hbm, upp_hbm, left_hbm, piece_hbm, out,
    low32, upp32, left_v, panel, low_hi, low_lo, upp_hi, upp_lo, left_d,
    p_hi, p_lo, h_hi, h_lo, solved, part,
    rp2, rq2, rx, fa1, fa3, rxp2, rxq2, fx2, fx1, fx3,
    loc_sem, ag_s, ag_r, par_s, par_r, rs_s, rs_r,
):
    y, xl, core, xh, z = coords()
    partner = device(y, xl, 1 - core, xh, z)
    across = device(y, 1 - xl, core, xh, z)
    ahead = device((y + 1 + 2 * core) % 4, xl, core, xh, z)
    behind = device((y + 3 + 2 * core) % 4, xl, core, xh, z)
    zp = device(y, xl, core, xh, (z + 1) % 4)
    zm = device(y, xl, core, xh, (z + 3) % 4)
    far = device(y, xl, core, 1 - xh, z)

    own = pltpu.make_async_copy(piece_hbm, panel.at[0, 0], loc_sem.at[0])
    own.start()
    loads = []
    for b in range(4):
        rows = pl.ds(b * TB, TB)
        cols = pl.ds(0, (b + 1) * TB)
        loads.append(pltpu.make_async_copy(low_hbm.at[rows, cols], low32.at[rows, cols], loc_sem.at[1 + b]))
    for b in range(4):
        rows = pl.ds(b * TB, TB)
        cols = pl.ds(b * TB, NI - b * TB)
        loads.append(pltpu.make_async_copy(upp_hbm.at[rows, cols], upp32.at[rows, cols], loc_sem.at[5 + b]))
    left_load = pltpu.make_async_copy(left_hbm, left_v, loc_sem.at[9])
    for copy in loads:
        copy.start()
    left_load.start()

    barrier = pltpu.get_barrier_semaphore()
    for peer in (partner, across, ahead, behind, zp, zm, far):
        pl.semaphore_signal(barrier, inc=1, device_id=peer, device_id_type=MESH)
    pl.semaphore_wait(barrier, 7)

    def link(n, src, dst, peer):
        return pltpu.make_async_remote_copy(
            src_ref=panel.at[src, 0], dst_ref=panel.at[dst, 0], send_sem=ag_s.at[n],
            recv_sem=ag_r.at[dst], device_id=peer, device_id_type=MESH)

    links = {
        1: link(0, 0, 1, ahead), 2: link(1, 0, 2, behind), 3: link(2, 0, 3, across), 4: link(3, 1, 4, ahead),
        5: link(4, 3, 5, ahead), 6: link(5, 3, 6, behind), 7: link(6, 6, 7, behind)}

    def share(i):
        return pltpu.make_async_remote_copy(
            src_ref=panel.at[i, 0], dst_ref=panel.at[i, 1], send_sem=par_s.at[i],
            recv_sem=par_r.at[i], device_id=partner, device_id_type=MESH)

    own.wait()
    share(0).start()
    links[1].start()
    links[3].start()

    strip = 32
    for b in range(4):
        loads[b].wait()

        @pl.loop(0, TB // strip)
        def _(s, b=b):
            rows = pl.ds(pl.multiple_of(b * TB + s * strip, strip), strip)
            cols = pl.ds(0, (b + 1) * TB)
            low_hi[rows, cols], low_lo[rows, cols] = split(low32[rows, cols])
    for b in range(4):
        loads[4 + b].wait()

        @pl.loop(0, TB // strip)
        def _(s, b=b):
            rows = pl.ds(pl.multiple_of(b * TB + s * strip, strip), strip)
            cols = pl.ds(b * TB, NI - b * TB)
            upp_hi[rows, cols], upp_lo[rows, cols] = split(upp32[rows, cols])

    left_load.wait()
    for dx in range(2):
        for dz in range(4):
            block = ((xh + dx) % 2) * 4 + (z + dz) % 4
            place = jnp.int32(0)
            touched = jnp.int32(0)
            for k in range(4):
                hit = ids[k] == block
                place = jnp.where(hit, k, place)
                touched = jnp.where(hit, 1, touched)
            left_d[dx, dz] = jnp.where(touched > 0, left_v[place], jnp.zeros((WB, NI), BF16))

    def reduce_copies(i):
        def send(n, src, dst, peer):
            return pltpu.make_async_remote_copy(
                src_ref=src, dst_ref=dst.at[i], send_sem=rs_s.at[i, n], recv_sem=rs_r.at[i, n],
                device_id=peer, device_id_type=MESH)

        both = slice(None)
        return {
            0: lambda: send(0, part.at[i, both, 2, A_UP], rp2, zp),
            1: lambda: send(1, part.at[i, both, 2, A_DN], rq2, zm),
            2: lambda: send(2, part.at[i, 1, both, X_ALL], rx, far),
            3: lambda: send(3, part.at[i, both, 1, A_ALL], fa1, zp),
            4: lambda: send(4, part.at[i, both, 3, A_ALL], fa3, zm),
            5: lambda: send(5, part.at[i, 0, 2, X_UP], rxp2, zp),
            6: lambda: send(6, part.at[i, 0, 2, X_DN], rxq2, zm),
            7: lambda: send(7, part.at[i, 1, 0, A_ALL], fx2, far),
            8: lambda: send(8, part.at[i, 0, 1, X_ALL], fx1, zp),
            9: lambda: send(9, part.at[i, 0, 3, X_ALL], fx3, zm),
        }

    def start(i, *which):
        copies = reduce_copies(i)
        for n in which:
            copies[n]().start()

    def arrive(i, *which):
        copies = reduce_copies(i)
        for n in which:
            copies[n]().wait_recv()

    def multiply(i):
        for h in range(2):
            @pl.loop(0, 8)
            def _(s, h=h):
                rows = pl.ds(pl.multiple_of(s * WB, WB), WB)
                cols = pl.ds(h * WB, WB)
                p_hi[rows, cols], p_lo[rows, cols] = split(panel[i, h, rows, :])

        def dot(a, b):
            return jnp.dot(a, b, preferred_element_type=F32)

        for b in range(4):
            rows, cols = pl.ds(b * TB, TB), pl.ds(0, (b + 1) * TB)
            a_hi = low_hi[rows, cols]
            half = dot(a_hi, p_hi[cols]) + dot(a_hi, p_lo[cols]) + dot(low_lo[rows, cols], p_hi[cols])
            h_hi[rows, :], h_lo[rows, :] = split(half)
        for b in range(4):
            rows, cols = pl.ds(b * TB, TB), pl.ds(b * TB, NI - b * TB)
            a_hi = upp_hi[rows, cols]
            full = dot(a_hi, h_hi[cols]) + dot(a_hi, h_lo[cols]) + dot(upp_lo[rows, cols], h_hi[cols])
            solved[rows, :] = full.astype(BF16)
        for dx in range(2):
            for dz in range(4):
                part[i, dx, dz] = dot(left_d[dx, dz], solved[...])

    def first(i):
        arrive(i, 0)
        part[i, :, 1, A_UP] += rp2[i]
        start(i, 3)
        arrive(i, 1)
        part[i, :, 3, A_DN] += rq2[i]
        start(i, 4)

    def second(i):
        arrive(i, 3, 4)
        part[i, :, 0, A_ALL] += fa1[i] + fa3[i]
        start(i, 7)

    def cross(i):
        arrive(i, 2)
        part[i, 0, :, X_ALL] += rx[i]
        start(i, 5, 6)

    def along(i):
        arrive(i, 5)
        part[i, 0, 1, X_UP] += rxp2[i]
        start(i, 8)
        arrive(i, 6)
        part[i, 0, 3, X_DN] += rxq2[i]
        start(i, 9)

    def finish(i):
        arrive(i, 7)
        out[i, A_ALL] = part[i, 0, 0, A_ALL] + fx2[i]
        arrive(i, 8, 9)
        out[i, X_ALL] = part[i, 0, 0, X_ALL] + (fx1[i] + fx3[i])

    def pass_on(a, *then):
        links[a].wait_recv()
        share(a).start()
        for n in then:
            links[n].start()

    @pl.loop(0, NCH)
    def _(step):
        @pl.when(step == 1)
        def _():
            pass_on(1)
            first(0)

        @pl.when(step == 2)
        def _():
            pass_on(2, 4)
            pass_on(3, 5, 6)
            first(1)

        @pl.when(step == 4)
        def _():
            first(3)
            pass_on(4)
            pass_on(5)

        @pl.when(step == 5)
        def _():
            pass_on(6, 7)

        @pl.when(step == 7)
        def _():
            pass_on(7)

        share(step).wait_recv()
        multiply(step)
        start(step, 0, 1, 2)

        @pl.when(step == 0)
        def _():
            links[1].wait_send()
            links[2].start()

        @pl.when((step == 3) | (step >= 5))
        def _():
            first(step - 1)

        for lag, stage in ((2, cross), (2, second), (3, along), (5, finish)):
            @pl.when(step >= lag)
            def _(lag=lag, stage=stage):
                stage(step - lag)

    for i, stage in (
        (6, cross), (7, first), (7, cross), (6, second), (5, along), (6, along), (7, second), (7, along),
        (3, finish), (4, finish), (5, finish), (6, finish), (7, finish),
    ):
        stage(i)

    for n in range(2, 8):
        links[n].wait_send()

    @pl.loop(0, NCH)
    def _(i):
        share(i).wait_send()
        for copy in reduce_copies(i).values():
            copy().wait_send()


def place_kernel(order, owned, base, out):
    y, xl, core, _, _ = coords()
    for j, (dy, dx) in enumerate(CHUNKS):
        for h in range(2):
            holder = (core + h) % 2
            source = ((y + 4 + dy * (1 - 2 * holder)) % 4) * 4 + ((xl + dx) % 2) * 2 + holder
            cols = pl.ds(pl.multiple_of(order[source] * WB, WB), WB)
            out[:, cols] = base[:, cols] - owned[j, :, h * WB:(h + 1) * WB]


def per_device(lower_inverse, upper_inverse, left_coupling, right_pieces, interface_block, a_gg, panel_order):
    vmem = pl.BlockSpec(memory_space=pltpu.VMEM)
    smem = pl.BlockSpec(memory_space=pltpu.SMEM)
    hbm = pl.BlockSpec(memory_space=pltpu.HBM)

    def buf(*shape, dtype=F32):
        return pltpu.VMEM(shape, dtype)

    dma = pltpu.SemaphoreType.DMA
    owned = pl.pallas_call(
        main_kernel,
        name="assemble",
        out_shape=jax.ShapeDtypeStruct((NCH, WB, CW), F32),
        in_specs=[smem, hbm, hbm, hbm, hbm],
        out_specs=vmem,
        scratch_shapes=[
            buf(NI, NI), buf(NI, NI), buf(4, WB, NI, dtype=BF16), buf(NCH, 2, NI, WB),
            buf(NI, NI, dtype=BF16), buf(NI, NI, dtype=BF16), buf(NI, NI, dtype=BF16), buf(NI, NI, dtype=BF16),
            buf(2, 4, WB, NI, dtype=BF16),
            buf(NI, CW, dtype=BF16), buf(NI, CW, dtype=BF16), buf(NI, CW, dtype=BF16), buf(NI, CW, dtype=BF16),
            buf(NI, CW, dtype=BF16), buf(NCH, 2, 4, WB, CW),
            buf(NCH, 2, UP, CW), buf(NCH, 2, DN, CW), buf(NCH, 4, XR, CW), buf(NCH, 2, RA, CW), buf(NCH, 2, RA, CW),
            buf(NCH, XU, CW), buf(NCH, XD, CW), buf(NCH, RA, CW), buf(NCH, XR, CW), buf(NCH, XR, CW),
            dma((10,)), dma((7,)), dma((NCH,)), dma((NCH,)), dma((NCH,)), dma((NCH, 10)), dma((NCH, 10)),
        ],
        compiler_params=pltpu.CompilerParams(
            collective_id=0, has_side_effects=True, vmem_limit_bytes=60 * 2**20),
    )(
        interface_block[0, 0], lower_inverse[0, 0], upper_inverse[0, 0],
        left_coupling[0, 0].reshape(4, WB, NI), right_pieces[0])
    schur = pl.pallas_call(
        place_kernel,
        name="place",
        out_shape=jax.ShapeDtypeStruct(a_gg.shape[1:], F32),
        in_specs=[smem, vmem, vmem],
        out_specs=vmem,
    )(panel_order, owned, a_gg[0])
    return schur[None]


def solution(mesh):
    return jax.shard_map(
        per_device,
        mesh=mesh,
        in_specs=(
            P("row", "col", None, None),
            P("row", "col", None, None),
            P("row", "col", None, None),
            P("col", None, "row"),
            P("row", "col", None),
            P("row", "col", None),
            P(),
        ),
        out_specs=P("row", "col", None),
        check_vma=False,
    )
```

```python
import functools

import jax
import jax.numpy as jnp
from jax import lax
from jax.experimental import pallas as pl
from jax.experimental.pallas import tpu as pltpu
from jax.sharding import PartitionSpec as P

MESH = pl.DeviceIdType.MESH
F32, BF16 = jnp.float32, jnp.bfloat16

NI = 1024
WB = 128
CW = 2 * WB
NCH = 8
TB = 256

UP, DN = 40, 32
XU, XD = 24, 32
RA = UP + DN
XR = XU + XD
A_UP, A_DN, A_ALL = pl.ds(0, UP), pl.ds(UP, DN), pl.ds(0, RA)
X_UP, X_DN, X_ALL = pl.ds(RA, XU), pl.ds(RA + XU, XD), pl.ds(RA, XR)

CHUNKS = ((0, 0), (-1, 0), (1, 0), (0, 1), (2, 0), (-1, 1), (1, 1), (2, 1))


def coords():
    r, c = lax.axis_index("row"), lax.axis_index("col")
    return r // 4, (r // 2) % 2, r % 2, c // 4, c % 4


def device(y, xl, core, xh, z):
    return (y * 4 + xl * 2 + core, xh * 4 + z)


def split(x):
    hi = x.astype(BF16)
    return hi, (x - hi.astype(F32)).astype(BF16)


def main_kernel(
    ids, order, low_hbm, upp_hbm, left_hbm, piece_hbm, base_hbm, out,
    low32, upp32, left_v, panel, low_hi, low_lo, upp_hi, upp_lo, left_d,
    p_hi, p_lo, h_hi, h_lo, solved, part,
    rp2, rq2, rx, fa1, fa3, rxp2, rxq2, fx2, fx1, fx3, base, total, origin,
    loc_sem, ag_s, ag_r, par_s, par_r, rs_s, rs_r,
):
    y, xl, core, xh, z = coords()
    partner = device(y, xl, 1 - core, xh, z)
    across = device(y, 1 - xl, core, xh, z)
    ahead = device((y + 1 + 2 * core) % 4, xl, core, xh, z)
    behind = device((y + 3 + 2 * core) % 4, xl, core, xh, z)
    zp = device(y, xl, core, xh, (z + 1) % 4)
    zm = device(y, xl, core, xh, (z + 3) % 4)
    far = device(y, xl, core, 1 - xh, z)

    own = pltpu.make_async_copy(piece_hbm, panel.at[0, 0], loc_sem.at[0])
    own.start()
    loads = []
    for b in range(4):
        rows = pl.ds(b * TB, TB)
        cols = pl.ds(0, (b + 1) * TB)
        loads.append(pltpu.make_async_copy(low_hbm.at[rows, cols], low32.at[rows, cols], loc_sem.at[1 + b]))
    for b in range(4):
        rows = pl.ds(b * TB, TB)
        cols = pl.ds(b * TB, NI - b * TB)
        loads.append(pltpu.make_async_copy(upp_hbm.at[rows, cols], upp32.at[rows, cols], loc_sem.at[5 + b]))
    left_load = pltpu.make_async_copy(left_hbm, left_v, loc_sem.at[9])
    for copy in loads:
        copy.start()
    left_load.start()
    base_load = pltpu.make_async_copy(base_hbm, base, loc_sem.at[10])
    base_load.start()

    barrier = pltpu.get_barrier_semaphore()
    for peer in (partner, across, ahead, behind, zp, zm, far):
        pl.semaphore_signal(barrier, inc=1, device_id=peer, device_id_type=MESH)
    pl.semaphore_wait(barrier, 7)

    def link(n, src, dst, peer):
        return pltpu.make_async_remote_copy(
            src_ref=panel.at[src, 0], dst_ref=panel.at[dst, 0], send_sem=ag_s.at[n],
            recv_sem=ag_r.at[dst], device_id=peer, device_id_type=MESH)

    links = {
        1: link(0, 0, 1, ahead), 2: link(1, 0, 2, behind), 3: link(2, 0, 3, across), 4: link(3, 1, 4, ahead),
        5: link(4, 3, 5, ahead), 6: link(5, 3, 6, behind), 7: link(6, 6, 7, behind)}

    def share(i):
        return pltpu.make_async_remote_copy(
            src_ref=panel.at[i, 0], dst_ref=panel.at[i, 1], send_sem=par_s.at[i],
            recv_sem=par_r.at[i], device_id=partner, device_id_type=MESH)

    own.wait()
    share(0).start()
    links[1].start()
    links[3].start()

    strip = 32
    for b in range(4):
        loads[b].wait()

        @pl.loop(0, TB // strip)
        def _(s, b=b):
            rows = pl.ds(pl.multiple_of(b * TB + s * strip, strip), strip)
            cols = pl.ds(0, (b + 1) * TB)
            low_hi[rows, cols], low_lo[rows, cols] = split(low32[rows, cols])
    for b in range(4):
        loads[4 + b].wait()

        @pl.loop(0, TB // strip)
        def _(s, b=b):
            rows = pl.ds(pl.multiple_of(b * TB + s * strip, strip), strip)
            cols = pl.ds(b * TB, NI - b * TB)
            upp_hi[rows, cols], upp_lo[rows, cols] = split(upp32[rows, cols])

    left_load.wait()
    for dx in range(2):
        for dz in range(4):
            block = ((xh + dx) % 2) * 4 + (z + dz) % 4
            place = jnp.int32(0)
            touched = jnp.int32(0)
            for k in range(4):
                hit = ids[k] == block
                place = jnp.where(hit, k, place)
                touched = jnp.where(hit, 1, touched)
            left_d[dx, dz] = jnp.where(touched > 0, left_v[place], jnp.zeros((WB, NI), BF16))

    def reduce_copies(i):
        def send(n, src, dst, peer):
            return pltpu.make_async_remote_copy(
                src_ref=src, dst_ref=dst.at[i], send_sem=rs_s.at[i, n], recv_sem=rs_r.at[i, n],
                device_id=peer, device_id_type=MESH)

        both = slice(None)
        return {
            0: lambda: send(0, part.at[i, both, 2, A_UP], rp2, zp),
            1: lambda: send(1, part.at[i, both, 2, A_DN], rq2, zm),
            2: lambda: send(2, part.at[i, 1, both, X_ALL], rx, far),
            3: lambda: send(3, part.at[i, both, 1, A_ALL], fa1, zp),
            4: lambda: send(4, part.at[i, both, 3, A_ALL], fa3, zm),
            5: lambda: send(5, part.at[i, 0, 2, X_UP], rxp2, zp),
            6: lambda: send(6, part.at[i, 0, 2, X_DN], rxq2, zm),
            7: lambda: send(7, part.at[i, 1, 0, A_ALL], fx2, far),
            8: lambda: send(8, part.at[i, 0, 1, X_ALL], fx1, zp),
            9: lambda: send(9, part.at[i, 0, 3, X_ALL], fx3, zm),
        }

    def start(i, *which):
        copies = reduce_copies(i)
        for n in which:
            copies[n]().start()

    def arrive(i, *which):
        copies = reduce_copies(i)
        for n in which:
            copies[n]().wait_recv()

    def multiply(i):
        for h in range(2):
            @pl.loop(0, 8)
            def _(s, h=h):
                rows = pl.ds(pl.multiple_of(s * WB, WB), WB)
                cols = pl.ds(h * WB, WB)
                p_hi[rows, cols], p_lo[rows, cols] = split(panel[i, h, rows, :])

        def dot(a, b):
            return jnp.dot(a, b, preferred_element_type=F32)

        for b in range(4):
            rows, cols = pl.ds(b * TB, TB), pl.ds(0, (b + 1) * TB)
            a_hi = low_hi[rows, cols]
            half = dot(a_hi, p_hi[cols]) + dot(a_hi, p_lo[cols]) + dot(low_lo[rows, cols], p_hi[cols])
            h_hi[rows, :], h_lo[rows, :] = split(half)
        for b in range(4):
            rows, cols = pl.ds(b * TB, TB), pl.ds(b * TB, NI - b * TB)
            a_hi = upp_hi[rows, cols]
            full = dot(a_hi, h_hi[cols]) + dot(a_hi, h_lo[cols]) + dot(upp_lo[rows, cols], h_hi[cols])
            solved[rows, :] = full.astype(BF16)
        for dx in range(2):
            for dz in range(4):
                part[i, dx, dz] = dot(left_d[dx, dz], solved[...])

    def first(i):
        arrive(i, 0)
        part[i, :, 1, A_UP] += rp2[i]
        start(i, 3)
        arrive(i, 1)
        part[i, :, 3, A_DN] += rq2[i]
        start(i, 4)

    def second(i):
        arrive(i, 3, 4)
        part[i, :, 0, A_ALL] += fa1[i] + fa3[i]
        start(i, 7)

    def cross(i):
        arrive(i, 2)
        part[i, 0, :, X_ALL] += rx[i]
        start(i, 5, 6)

    def along(i):
        arrive(i, 5)
        part[i, 0, 1, X_UP] += rxp2[i]
        start(i, 8)
        arrive(i, 6)
        part[i, 0, 3, X_DN] += rxq2[i]
        start(i, 9)

    def finish(i):
        arrive(i, 7)
        rows = part[i, 0, 0, A_ALL] + fx2[i]
        for h in range(2):
            total[2 * i + h, A_ALL] = rows[:, h * WB:(h + 1) * WB]
        arrive(i, 8, 9)
        rows = part[i, 0, 0, X_ALL] + (fx1[i] + fx3[i])
        for h in range(2):
            total[2 * i + h, X_ALL] = rows[:, h * WB:(h + 1) * WB]

    def pass_on(a, *then):
        links[a].wait_recv()
        share(a).start()
        for n in then:
            links[n].start()

    @pl.loop(0, NCH)
    def _(step):
        @pl.when(step == 1)
        def _():
            pass_on(1)
            first(0)

        @pl.when(step == 2)
        def _():
            pass_on(2, 4)
            pass_on(3, 5, 6)
            first(1)

        @pl.when(step == 4)
        def _():
            first(3)
            pass_on(4)
            pass_on(5)

        @pl.when(step == 5)
        def _():
            pass_on(6, 7)

        @pl.when(step == 7)
        def _():
            pass_on(7)

        share(step).wait_recv()
        multiply(step)
        start(step, 0, 1, 2)

        @pl.when(step == 0)
        def _():
            links[1].wait_send()
            links[2].start()

        @pl.when((step == 3) | (step >= 5))
        def _():
            first(step - 1)

        for lag, stage in ((2, cross), (2, second), (3, along), (5, finish)):
            @pl.when(step >= lag)
            def _(lag=lag, stage=stage):
                stage(step - lag)

    base_load.wait()
    places = []
    for dy, dx in CHUNKS:
        for h in range(2):
            holder = (core + h) % 2
            places.append(order[((y + 4 + dy * (1 - 2 * holder)) % 4) * 4 + ((xl + dx) % 2) * 2 + holder])
    for p in range(2 * NCH):
        found = jnp.int32(0)
        for t in range(2 * NCH):
            found = jnp.where(places[t] == p, t, found)
        origin[p] = found

    for i, stage in (
        (6, cross), (7, first), (7, cross), (6, second), (5, along), (6, along), (7, second), (7, along),
        (3, finish), (4, finish), (5, finish), (6, finish), (7, finish),
    ):
        stage(i)

    for p in range(2 * NCH):
        cols = slice(p * WB, (p + 1) * WB)
        out[:, cols] = base[:, cols] - total[origin[p]]

    for n in range(2, 8):
        links[n].wait_send()

    @pl.loop(0, NCH)
    def _(i):
        share(i).wait_send()
        for copy in reduce_copies(i).values():
            copy().wait_send()


def per_device(lower_inverse, upper_inverse, left_coupling, right_pieces, interface_block, a_gg, panel_order):
    vmem = pl.BlockSpec(memory_space=pltpu.VMEM)
    smem = pl.BlockSpec(memory_space=pltpu.SMEM)
    hbm = pl.BlockSpec(memory_space=pltpu.HBM)

    def buf(*shape, dtype=F32):
        return pltpu.VMEM(shape, dtype)

    def fixed(x):
        return pltpu.with_memory_space_constraint(x, pltpu.HBM)

    dma = pltpu.SemaphoreType.DMA
    schur = pl.pallas_call(
        main_kernel,
        name="assemble",
        out_shape=jax.ShapeDtypeStruct(a_gg.shape[1:], F32),
        in_specs=[smem, smem, hbm, hbm, hbm, hbm, hbm],
        out_specs=vmem,
        scratch_shapes=[
            buf(NI, NI), buf(NI, NI), buf(4, WB, NI, dtype=BF16), buf(NCH, 2, NI, WB),
            buf(NI, NI, dtype=BF16), buf(NI, NI, dtype=BF16), buf(NI, NI, dtype=BF16), buf(NI, NI, dtype=BF16),
            buf(2, 4, WB, NI, dtype=BF16),
            buf(NI, CW, dtype=BF16), buf(NI, CW, dtype=BF16), buf(NI, CW, dtype=BF16), buf(NI, CW, dtype=BF16),
            buf(NI, CW, dtype=BF16), buf(NCH, 2, 4, WB, CW),
            buf(NCH, 2, UP, CW), buf(NCH, 2, DN, CW), buf(NCH, 4, XR, CW), buf(NCH, 2, RA, CW), buf(NCH, 2, RA, CW),
            buf(NCH, XU, CW), buf(NCH, XD, CW), buf(NCH, RA, CW), buf(NCH, XR, CW), buf(NCH, XR, CW),
            buf(WB, a_gg.shape[2]), buf(2 * NCH, WB, WB), pltpu.SMEM((2 * NCH,), jnp.int32),
            dma((11,)), dma((7,)), dma((NCH,)), dma((NCH,)), dma((NCH,)), dma((NCH, 10)), dma((NCH, 10)),
        ],
        compiler_params=pltpu.CompilerParams(
            collective_id=0, has_side_effects=True, vmem_limit_bytes=52 * 2**20),
    )(
        fixed(interface_block[0, 0]), fixed(panel_order), fixed(lower_inverse[0, 0]), fixed(upper_inverse[0, 0]),
        fixed(left_coupling[0, 0].reshape(4, WB, NI)), fixed(right_pieces[0]), fixed(a_gg[0]))
    return schur[None]


def solution(mesh):
    return jax.shard_map(
        per_device,
        mesh=mesh,
        in_specs=(
            P("row", "col", None, None),
            P("row", "col", None, None),
            P("row", "col", None, None),
            P("col", None, "row"),
            P("row", "col", None),
            P("row", "col", None),
            P(),
        ),
        out_specs=P("row", "col", None),
        check_vma=False,
    )
```

```python
import functools

import jax
import jax.numpy as jnp
from jax import lax
from jax.experimental import pallas as pl
from jax.experimental.pallas import tpu as pltpu
from jax.sharding import PartitionSpec as P

MESH = pl.DeviceIdType.MESH
F32, BF16 = jnp.float32, jnp.bfloat16

NI = 1024
WB = 128
CW = 2 * WB
NCH = 8
TB = 256

UP, DN = 40, 32
XU, XD = 24, 32
RA = UP + DN
XR = XU + XD
A_UP, A_DN, A_ALL = pl.ds(0, UP), pl.ds(UP, DN), pl.ds(0, RA)
X_UP, X_DN, X_ALL = pl.ds(RA, XU), pl.ds(RA + XU, XD), pl.ds(RA, XR)

CHUNKS = ((0, 0), (-1, 0), (1, 0), (0, 1), (2, 0), (-1, 1), (1, 1), (2, 1))


def coords():
    r, c = lax.axis_index("row"), lax.axis_index("col")
    return r // 4, (r // 2) % 2, r % 2, c // 4, c % 4


def device(y, xl, core, xh, z):
    return (y * 4 + xl * 2 + core, xh * 4 + z)


def split(x):
    hi = x.astype(BF16)
    return hi, (x - hi.astype(F32)).astype(BF16)


def main_kernel(
    ids, order, low_hbm, upp_hbm, left_hbm, piece_hbm, base_hbm, out,
    low32, upp32, left_v, panel, low_hi, low_lo, upp_hi, upp_lo, left_d,
    p_hi, p_lo, h_hi, h_lo, solved, part,
    rp2, rq2, rx, fa1, fa3, rxp2, rxq2, fx2, fx1, fx3, base, total, origin,
    loc_sem, ag_s, ag_r, par_s, par_r, rs_s, rs_r,
):
    y, xl, core, xh, z = coords()
    partner = device(y, xl, 1 - core, xh, z)
    across = device(y, 1 - xl, core, xh, z)
    ahead = device((y + 1 + 2 * core) % 4, xl, core, xh, z)
    behind = device((y + 3 + 2 * core) % 4, xl, core, xh, z)
    zp = device(y, xl, core, xh, (z + 1) % 4)
    zm = device(y, xl, core, xh, (z + 3) % 4)
    far = device(y, xl, core, 1 - xh, z)

    own = pltpu.make_async_copy(piece_hbm, panel.at[0, 0], loc_sem.at[0])
    own.start()
    loads = []
    for b in range(4):
        rows = pl.ds(b * TB, TB)
        cols = pl.ds(0, (b + 1) * TB)
        loads.append(pltpu.make_async_copy(low_hbm.at[rows, cols], low32.at[rows, cols], loc_sem.at[1 + b]))
    for b in range(4):
        rows = pl.ds(b * TB, TB)
        cols = pl.ds(b * TB, NI - b * TB)
        loads.append(pltpu.make_async_copy(upp_hbm.at[rows, cols], upp32.at[rows, cols], loc_sem.at[5 + b]))
    left_load = pltpu.make_async_copy(left_hbm, left_v, loc_sem.at[9])
    for copy in loads:
        copy.start()
    left_load.start()
    base_load = pltpu.make_async_copy(base_hbm, base, loc_sem.at[10])
    base_load.start()

    barrier = pltpu.get_barrier_semaphore()
    for peer in (partner, across, ahead, behind, zp, zm, far):
        pl.semaphore_signal(barrier, inc=1, device_id=peer, device_id_type=MESH)
    pl.semaphore_wait(barrier, 7)

    def link(n, src, dst, peer):
        return pltpu.make_async_remote_copy(
            src_ref=panel.at[src, 0], dst_ref=panel.at[dst, 0], send_sem=ag_s.at[n],
            recv_sem=ag_r.at[dst], device_id=peer, device_id_type=MESH)

    links = {
        1: link(0, 0, 1, ahead), 2: link(1, 0, 2, behind), 3: link(2, 0, 3, across), 4: link(3, 1, 4, ahead),
        5: link(4, 3, 5, ahead), 6: link(5, 3, 6, behind), 7: link(6, 6, 7, behind)}

    def share(i, at=None):
        return pltpu.make_async_remote_copy(
            src_ref=panel.at[i, 0], dst_ref=panel.at[i, 1], send_sem=par_s,
            recv_sem=par_r.at[i if at is None else at], device_id=partner, device_id_type=MESH)

    own.wait()
    share(0).start()
    links[1].start()
    links[3].start()

    strip = 32
    for b in range(4):
        loads[b].wait()

        @pl.loop(0, TB // strip)
        def _(s, b=b):
            rows = pl.ds(pl.multiple_of(b * TB + s * strip, strip), strip)
            cols = pl.ds(0, (b + 1) * TB)
            low_hi[rows, cols], low_lo[rows, cols] = split(low32[rows, cols])
    for b in range(4):
        loads[4 + b].wait()

        @pl.loop(0, TB // strip)
        def _(s, b=b):
            rows = pl.ds(pl.multiple_of(b * TB + s * strip, strip), strip)
            cols = pl.ds(b * TB, NI - b * TB)
            upp_hi[rows, cols], upp_lo[rows, cols] = split(upp32[rows, cols])

    left_load.wait()
    for dx in range(2):
        for dz in range(4):
            block = ((xh + dx) % 2) * 4 + (z + dz) % 4
            place = jnp.int32(0)
            touched = jnp.int32(0)
            for k in range(4):
                hit = ids[k] == block
                place = jnp.where(hit, k, place)
                touched = jnp.where(hit, 1, touched)
            left_d[dx, dz * WB:(dz + 1) * WB] = jnp.where(touched > 0, left_v[place], jnp.zeros((WB, NI), BF16))

    def reduce_copies(i, at=None):
        at = i if at is None else at

        def send(n, src, dst, peer):
            return pltpu.make_async_remote_copy(
                src_ref=src, dst_ref=dst.at[i], send_sem=rs_s.at[n], recv_sem=rs_r.at[at, n],
                device_id=peer, device_id_type=MESH)

        both = slice(None)
        return {
            0: lambda: send(0, part.at[i, both, 2, A_UP], rp2, zp),
            1: lambda: send(1, part.at[i, both, 2, A_DN], rq2, zm),
            2: lambda: send(2, part.at[i, 1, both, X_ALL], rx, far),
            3: lambda: send(3, part.at[i, 1, 1, A_ALL], fa1.at[1], zp),
            4: lambda: send(4, part.at[i, 1, 3, A_ALL], fa3.at[1], zm),
            10: lambda: send(10, part.at[i, 0, 1, A_ALL], fa1.at[0], zp),
            11: lambda: send(11, part.at[i, 0, 3, A_ALL], fa3.at[0], zm),
            5: lambda: send(5, part.at[i, 0, 2, X_UP], rxp2, zp),
            6: lambda: send(6, part.at[i, 0, 2, X_DN], rxq2, zm),
            7: lambda: send(7, part.at[i, 1, 0, A_ALL], fx2, far),
            8: lambda: send(8, part.at[i, 0, 1, X_ALL], fx1, zp),
            9: lambda: send(9, part.at[i, 0, 3, X_ALL], fx3, zm),
        }

    def start(i, *which):
        copies = reduce_copies(i)
        for n in which:
            copies[n]().start()

    def arrive(i, *which):
        copies = reduce_copies(i)
        for n in which:
            copies[n]().wait_recv()

    def multiply(i):
        for h in range(2):
            @pl.loop(0, 8)
            def _(s, h=h):
                rows = pl.ds(pl.multiple_of(s * WB, WB), WB)
                cols = pl.ds(h * WB, WB)
                p_hi[rows, cols], p_lo[rows, cols] = split(panel[i, h, rows, :])

        def dot(a, b):
            return jnp.dot(a, b, preferred_element_type=F32)

        for b in range(4):
            rows, cols = pl.ds(b * TB, TB), pl.ds(0, (b + 1) * TB)
            a_hi = low_hi[rows, cols]
            both = dot(jnp.concatenate([a_hi, low_lo[rows, cols]], axis=0), p_hi[cols])
            half = both[:TB] + both[TB:] + dot(a_hi, p_lo[cols])
            h_hi[rows, :], h_lo[rows, :] = split(half)
        for b in range(4):
            rows, cols = pl.ds(b * TB, TB), pl.ds(b * TB, NI - b * TB)
            a_hi = upp_hi[rows, cols]
            both = dot(jnp.concatenate([a_hi, upp_lo[rows, cols]], axis=0), h_hi[cols])
            full = both[:TB] + both[TB:] + dot(a_hi, h_lo[cols])
            solved[rows, :] = full.astype(BF16)
        for dx in range(2):
            part[i, dx] = dot(left_d[dx], solved[...]).reshape(4, WB, CW)

    def first(i):
        arrive(i, 0)
        part[i, :, 1, A_UP] += rp2[i]
        start(i, 3, 10)
        arrive(i, 1)
        part[i, :, 3, A_DN] += rq2[i]
        start(i, 4, 11)

    def second(i):
        arrive(i, 3, 4)
        part[i, 1, 0, A_ALL] += fa1[1, i] + fa3[1, i]
        start(i, 7)

    def cross(i):
        arrive(i, 2)
        part[i, 0, :, X_ALL] += rx[i]
        start(i, 5, 6)

    def along(i):
        arrive(i, 5)
        part[i, 0, 1, X_UP] += rxp2[i]
        start(i, 8)
        arrive(i, 6)
        part[i, 0, 3, X_DN] += rxq2[i]
        start(i, 9)

    def finish(i):
        arrive(i, 10, 11, 7)
        rows = part[i, 0, 0, A_ALL] + (fa1[0, i] + fa3[0, i]) + fx2[i]
        for h in range(2):
            total[2 * i + h, A_ALL] = rows[:, h * WB:(h + 1) * WB]
        arrive(i, 8, 9)
        rows = part[i, 0, 0, X_ALL] + (fx1[i] + fx3[i])
        for h in range(2):
            total[2 * i + h, X_ALL] = rows[:, h * WB:(h + 1) * WB]

    def pass_on(a, *then):
        links[a].wait_recv()
        share(a).start()
        for n in then:
            links[n].start()

    @pl.loop(0, NCH)
    def _(step):
        @pl.when(step == 1)
        def _():
            pass_on(1)
            first(0)

        @pl.when(step == 2)
        def _():
            links[4].start()
            pass_on(2)
            pass_on(3, 5, 6)
            first(1)

        @pl.when(step == 4)
        def _():
            first(3)
            pass_on(4)
            pass_on(6, 7)

        @pl.when(step == 5)
        def _():
            pass_on(5)
            first(4)

        @pl.when(step == 6)
        def _():
            pass_on(7)

        share(step).wait_recv()
        multiply(step)
        start(step, 0, 1, 2)

        @pl.when(step == 0)
        def _():
            links[1].wait_send()
            links[2].start()

        @pl.when((step == 3) | (step >= 6))
        def _():
            first(step - 1)

        for lag, stage in ((2, cross), (2, second), (3, along), (5, finish)):
            @pl.when(step >= lag)
            def _(lag=lag, stage=stage):
                stage(step - lag)

    base_load.wait()
    places = []
    for dy, dx in CHUNKS:
        for h in range(2):
            holder = (core + h) % 2
            places.append(order[((y + 4 + dy * (1 - 2 * holder)) % 4) * 4 + ((xl + dx) % 2) * 2 + holder])
    for p in range(2 * NCH):
        found = jnp.int32(0)
        for t in range(2 * NCH):
            found = jnp.where(places[t] == p, t, found)
        origin[p] = found

    for i, stage in (
        (6, cross), (7, first), (7, cross), (6, second), (5, along), (6, along), (7, second), (7, along),
        (3, finish), (4, finish), (5, finish), (6, finish), (7, finish),
    ):
        stage(i)

    for p in range(2 * NCH):
        cols = slice(p * WB, (p + 1) * WB)
        out[:, cols] = base[:, cols] - total[origin[p]]

    for n in range(2, 8):
        links[n].wait_send()
    every = slice(None)
    share(every, 0).wait_send()
    for copy in reduce_copies(every, 0).values():
        copy().wait_send()


def per_device(lower_inverse, upper_inverse, left_coupling, right_pieces, interface_block, a_gg, panel_order):
    vmem = pl.BlockSpec(memory_space=pltpu.VMEM)
    smem = pl.BlockSpec(memory_space=pltpu.SMEM)
    hbm = pl.BlockSpec(memory_space=pltpu.HBM)

    def buf(*shape, dtype=F32):
        return pltpu.VMEM(shape, dtype)

    def fixed(x):
        return pltpu.with_memory_space_constraint(x, pltpu.HBM)

    dma = pltpu.SemaphoreType.DMA
    schur = pl.pallas_call(
        main_kernel,
        name="assemble",
        out_shape=jax.ShapeDtypeStruct(a_gg.shape[1:], F32),
        in_specs=[smem, smem, hbm, hbm, hbm, hbm, hbm],
        out_specs=vmem,
        scratch_shapes=[
            buf(NI, NI), buf(NI, NI), buf(4, WB, NI, dtype=BF16), buf(NCH, 2, NI, WB),
            buf(NI, NI, dtype=BF16), buf(NI, NI, dtype=BF16), buf(NI, NI, dtype=BF16), buf(NI, NI, dtype=BF16),
            buf(2, 4 * WB, NI, dtype=BF16),
            buf(NI, CW, dtype=BF16), buf(NI, CW, dtype=BF16), buf(NI, CW, dtype=BF16), buf(NI, CW, dtype=BF16),
            buf(NI, CW, dtype=BF16), buf(NCH, 2, 4, WB, CW),
            buf(NCH, 2, UP, CW), buf(NCH, 2, DN, CW), buf(NCH, 4, XR, CW), buf(2, NCH, RA, CW), buf(2, NCH, RA, CW),
            buf(NCH, XU, CW), buf(NCH, XD, CW), buf(NCH, RA, CW), buf(NCH, XR, CW), buf(NCH, XR, CW),
            buf(WB, a_gg.shape[2]), buf(2 * NCH, WB, WB), pltpu.SMEM((2 * NCH,), jnp.int32),
            dma((11,)), dma((7,)), dma((NCH,)), dma, dma((NCH,)), dma((12,)), dma((NCH, 12)),
        ],
        compiler_params=pltpu.CompilerParams(
            collective_id=0, has_side_effects=True, vmem_limit_bytes=52 * 2**20),
    )(
        fixed(interface_block[0, 0]), fixed(panel_order), fixed(lower_inverse[0, 0]), fixed(upper_inverse[0, 0]),
        fixed(left_coupling[0, 0].reshape(4, WB, NI)), fixed(right_pieces[0]), fixed(a_gg[0]))
    return schur[None]


def solution(mesh):
    return jax.shard_map(
        per_device,
        mesh=mesh,
        in_specs=(
            P("row", "col", None, None),
            P("row", "col", None, None),
            P("row", "col", None, None),
            P("col", None, "row"),
            P("row", "col", None),
            P("row", "col", None),
            P(),
        ),
        out_specs=P("row", "col", None),
        check_vma=False,
    )
```

```python
import functools

import jax
import jax.numpy as jnp
from jax import lax
from jax.experimental import pallas as pl
from jax.experimental.pallas import tpu as pltpu
from jax.sharding import PartitionSpec as P

MESH = pl.DeviceIdType.MESH
F32, BF16 = jnp.float32, jnp.bfloat16

NI = 1024
WB = 128
CW = 2 * WB
NCH = 8
TB = 256

UP, DN = 40, 32
XU, XD = 24, 32
RA = UP + DN
XR = XU + XD
A_UP, A_DN, A_ALL = pl.ds(0, UP), pl.ds(UP, DN), pl.ds(0, RA)
X_UP, X_DN, X_ALL = pl.ds(RA, XU), pl.ds(RA + XU, XD), pl.ds(RA, XR)

CHUNKS = ((0, 0), (-1, 0), (1, 0), (0, 1), (2, 0), (-1, 1), (1, 1), (2, 1))

LEFT_ORDER = tuple((dz, dx) for dz in (2, 1, 3, 0) for dx in (0, 1))


def coords():
    r, c = lax.axis_index("row"), lax.axis_index("col")
    return r // 4, (r // 2) % 2, r % 2, c // 4, c % 4


def device(y, xl, core, xh, z):
    return (y * 4 + xl * 2 + core, xh * 4 + z)


def split(x):
    hi = x.astype(BF16)
    return hi, (x - hi.astype(F32)).astype(BF16)


def main_kernel(
    ids, order, low_hbm, upp_hbm, left_hbm, piece_hbm, base_hbm, out,
    low32, upp32, left_v, panel, low_hi, low_lo, upp_hi, upp_lo, left_d,
    p_hi, p_lo, h_hi, h_lo, solved, part,
    rp2, rq2, rx, up1, dn3, dn1, up3, rxp2, rxq2, fx2, fx1, fx3, base, total, origin,
    loc_sem, ag_s, ag_r, par_s, par_r, rs_s, rs_r,
):
    y, xl, core, xh, z = coords()
    partner = device(y, xl, 1 - core, xh, z)
    across = device(y, 1 - xl, core, xh, z)
    ahead = device((y + 1 + 2 * core) % 4, xl, core, xh, z)
    behind = device((y + 3 + 2 * core) % 4, xl, core, xh, z)
    zp = device(y, xl, core, xh, (z + 1) % 4)
    zm = device(y, xl, core, xh, (z + 3) % 4)
    far = device(y, xl, core, 1 - xh, z)

    own = pltpu.make_async_copy(piece_hbm, panel.at[0, 0], loc_sem.at[0])
    own.start()
    loads = []
    for b in range(4):
        rows = pl.ds(b * TB, TB)
        cols = pl.ds(0, (b + 1) * TB)
        loads.append(pltpu.make_async_copy(low_hbm.at[rows, cols], low32.at[rows, cols], loc_sem.at[1 + b]))
    for b in range(4):
        rows = pl.ds(b * TB, TB)
        cols = pl.ds(b * TB, NI - b * TB)
        loads.append(pltpu.make_async_copy(upp_hbm.at[rows, cols], upp32.at[rows, cols], loc_sem.at[5 + b]))
    left_load = pltpu.make_async_copy(left_hbm, left_v, loc_sem.at[9])
    for copy in loads:
        copy.start()
    left_load.start()
    base_load = pltpu.make_async_copy(base_hbm, base, loc_sem.at[10])
    base_load.start()

    barrier = pltpu.get_barrier_semaphore()
    for peer in (partner, across, ahead, behind, zp, zm, far):
        pl.semaphore_signal(barrier, inc=1, device_id=peer, device_id_type=MESH)
    pl.semaphore_wait(barrier, 7)

    def link(n, src, dst, peer):
        return pltpu.make_async_remote_copy(
            src_ref=panel.at[src, 0], dst_ref=panel.at[dst, 0], send_sem=ag_s.at[n],
            recv_sem=ag_r.at[dst], device_id=peer, device_id_type=MESH)

    links = {
        1: link(0, 0, 1, ahead), 2: link(1, 0, 2, behind), 3: link(2, 0, 3, across), 4: link(3, 1, 4, ahead),
        5: link(4, 3, 5, ahead), 6: link(5, 3, 6, behind), 7: link(6, 6, 7, behind)}

    def share(i, at=None):
        return pltpu.make_async_remote_copy(
            src_ref=panel.at[i, 0], dst_ref=panel.at[i, 1], send_sem=par_s,
            recv_sem=par_r.at[i if at is None else at], device_id=partner, device_id_type=MESH)

    own.wait()
    share(0).start()
    links[1].start()
    links[3].start()

    strip = 32
    for b in range(4):
        loads[b].wait()

        @pl.loop(0, TB // strip)
        def _(s, b=b):
            rows = pl.ds(pl.multiple_of(b * TB + s * strip, strip), strip)
            cols = pl.ds(0, (b + 1) * TB)
            low_hi[rows, cols], low_lo[rows, cols] = split(low32[rows, cols])
    for b in range(4):
        loads[4 + b].wait()

        @pl.loop(0, TB // strip)
        def _(s, b=b):
            rows = pl.ds(pl.multiple_of(b * TB + s * strip, strip), strip)
            cols = pl.ds(b * TB, NI - b * TB)
            upp_hi[rows, cols], upp_lo[rows, cols] = split(upp32[rows, cols])

    left_load.wait()
    for n, (dz, dx) in enumerate(LEFT_ORDER):
        block = ((xh + dx) % 2) * 4 + (z + dz) % 4
        place = jnp.int32(0)
        touched = jnp.int32(0)
        for k in range(4):
            hit = ids[k] == block
            place = jnp.where(hit, k, place)
            touched = jnp.where(hit, 1, touched)
        left_d[n * WB:(n + 1) * WB] = jnp.where(touched > 0, left_v[place], jnp.zeros((WB, NI), BF16))

    def reduce_copies(i, at=None):
        at = i if at is None else at

        def send(n, src, dst, peer):
            return pltpu.make_async_remote_copy(
                src_ref=src, dst_ref=dst.at[i], send_sem=rs_s.at[n], recv_sem=rs_r.at[at, n],
                device_id=peer, device_id_type=MESH)

        both = slice(None)
        return {
            0: lambda: send(0, part.at[i, both, 2, A_UP], rp2, zp),
            1: lambda: send(1, part.at[i, both, 2, A_DN], rq2, zm),
            2: lambda: send(2, part.at[i, 1, both, X_ALL], rx, far),
            3: lambda: send(3, part.at[i, 1, 1, A_UP], up1.at[1], zp),
            4: lambda: send(4, part.at[i, 1, 3, A_DN], dn3.at[1], zm),
            10: lambda: send(10, part.at[i, 0, 1, A_UP], up1.at[0], zp),
            11: lambda: send(11, part.at[i, 0, 3, A_DN], dn3.at[0], zm),
            12: lambda: send(12, part.at[i, both, 1, A_DN], dn1, zp),
            13: lambda: send(13, part.at[i, both, 3, A_UP], up3, zm),
            5: lambda: send(5, part.at[i, 0, 2, X_UP], rxp2, zp),
            6: lambda: send(6, part.at[i, 0, 2, X_DN], rxq2, zm),
            7: lambda: send(7, part.at[i, 1, 0, A_ALL], fx2, far),
            8: lambda: send(8, part.at[i, 0, 1, X_ALL], fx1, zp),
            9: lambda: send(9, part.at[i, 0, 3, X_ALL], fx3, zm),
        }

    def start(i, *which):
        copies = reduce_copies(i)
        for n in which:
            copies[n]().start()

    def arrive(i, *which):
        copies = reduce_copies(i)
        for n in which:
            copies[n]().wait_recv()

    def multiply(i):
        for h in range(2):
            @pl.loop(0, 8)
            def _(s, h=h):
                rows = pl.ds(pl.multiple_of(s * WB, WB), WB)
                cols = pl.ds(h * WB, WB)
                p_hi[rows, cols], p_lo[rows, cols] = split(panel[i, h, rows, :])

        def dot(a, b):
            return jnp.dot(a, b, preferred_element_type=F32)

        for b in range(4):
            rows, cols = pl.ds(b * TB, TB), pl.ds(0, (b + 1) * TB)
            a_hi = low_hi[rows, cols]
            both = dot(jnp.concatenate([a_hi, low_lo[rows, cols]], axis=0), p_hi[cols])
            half = both[:TB] + both[TB:] + dot(a_hi, p_lo[cols])
            h_hi[rows, :], h_lo[rows, :] = split(half)
        for b in range(4):
            rows, cols = pl.ds(b * TB, TB), pl.ds(b * TB, NI - b * TB)
            a_hi = upp_hi[rows, cols]
            both = dot(jnp.concatenate([a_hi, upp_lo[rows, cols]], axis=0), h_hi[cols])
            full = both[:TB] + both[TB:] + dot(a_hi, h_lo[cols])
            solved[rows, :] = full.astype(BF16)
        for first_n in (0, 4):
            blocks = dot(left_d[first_n * WB:(first_n + 4) * WB], solved[...]).reshape(4, WB, CW)
            for n in range(4):
                dz, dx = LEFT_ORDER[first_n + n]
                part[i, dx, dz] = blocks[n]
        start(i, 0, 1, 12, 13, 2)

    def first(i):
        arrive(i, 0)
        part[i, :, 1, A_UP] += rp2[i]
        start(i, 3, 10)
        arrive(i, 1)
        part[i, :, 3, A_DN] += rq2[i]
        start(i, 4, 11)

    def second(i):
        arrive(i, 12, 13, 3, 4)
        part[i, 1, 0, A_UP] += up1[1, i] + up3[i, 1]
        part[i, 1, 0, A_DN] += dn1[i, 1] + dn3[1, i]
        start(i, 7)

    def cross(i):
        arrive(i, 2)
        part[i, 0, :, X_ALL] += rx[i]
        start(i, 5, 6)

    def along(i):
        arrive(i, 5)
        part[i, 0, 1, X_UP] += rxp2[i]
        start(i, 8)
        arrive(i, 6)
        part[i, 0, 3, X_DN] += rxq2[i]
        start(i, 9)

    def finish(i):
        arrive(i, 10, 11, 7)
        for rows, others in (
            (A_UP, up1[0, i] + up3[i, 0] + fx2[i, 0:UP]),
            (A_DN, dn1[i, 0] + dn3[0, i] + fx2[i, UP:RA]),
        ):
            summed = part[i, 0, 0, rows] + others
            for h in range(2):
                total[2 * i + h, rows] = summed[:, h * WB:(h + 1) * WB]
        arrive(i, 8, 9)
        rows = part[i, 0, 0, X_ALL] + (fx1[i] + fx3[i])
        for h in range(2):
            total[2 * i + h, X_ALL] = rows[:, h * WB:(h + 1) * WB]

    def pass_on(a, *then):
        links[a].wait_recv()
        share(a).start()
        for n in then:
            links[n].start()

    @pl.loop(0, NCH)
    def _(step):
        @pl.when(step == 1)
        def _():
            pass_on(1)
            first(0)

        @pl.when(step == 2)
        def _():
            links[4].start()
            pass_on(2)
            pass_on(3, 5, 6)
            first(1)

        @pl.when(step == 4)
        def _():
            first(3)
            pass_on(4)
            pass_on(6, 7)

        @pl.when(step == 5)
        def _():
            pass_on(5)
            first(4)

        @pl.when(step == 6)
        def _():
            pass_on(7)

        share(step).wait_recv()
        multiply(step)

        @pl.when(step == 0)
        def _():
            links[1].wait_send()
            links[2].start()

        @pl.when((step == 3) | (step >= 6))
        def _():
            first(step - 1)

        for lag, stage in ((2, cross), (2, second), (3, along), (5, finish)):
            @pl.when(step >= lag)
            def _(lag=lag, stage=stage):
                stage(step - lag)

    base_load.wait()
    places = []
    for dy, dx in CHUNKS:
        for h in range(2):
            holder = (core + h) % 2
            places.append(order[((y + 4 + dy * (1 - 2 * holder)) % 4) * 4 + ((xl + dx) % 2) * 2 + holder])
    for p in range(2 * NCH):
        found = jnp.int32(0)
        for t in range(2 * NCH):
            found = jnp.where(places[t] == p, t, found)
        origin[p] = found

    for i, stage in (
        (6, cross), (7, first), (7, cross), (6, second), (5, along), (6, along), (7, second), (7, along),
        (3, finish), (4, finish), (5, finish), (6, finish), (7, finish),
    ):
        stage(i)

    for p in range(2 * NCH):
        cols = slice(p * WB, (p + 1) * WB)
        out[:, cols] = base[:, cols] - total[origin[p]]

    for n in range(2, 8):
        links[n].wait_send()
    every = slice(None)
    share(every, 0).wait_send()
    for copy in reduce_copies(every, 0).values():
        copy().wait_send()


def per_device(lower_inverse, upper_inverse, left_coupling, right_pieces, interface_block, a_gg, panel_order):
    vmem = pl.BlockSpec(memory_space=pltpu.VMEM)
    smem = pl.BlockSpec(memory_space=pltpu.SMEM)
    hbm = pl.BlockSpec(memory_space=pltpu.HBM)

    def buf(*shape, dtype=F32):
        return pltpu.VMEM(shape, dtype)

    def fixed(x):
        return pltpu.with_memory_space_constraint(x, pltpu.HBM)

    dma = pltpu.SemaphoreType.DMA
    schur = pl.pallas_call(
        main_kernel,
        name="assemble",
        out_shape=jax.ShapeDtypeStruct(a_gg.shape[1:], F32),
        in_specs=[smem, smem, hbm, hbm, hbm, hbm, hbm],
        out_specs=vmem,
        scratch_shapes=[
            buf(NI, NI), buf(NI, NI), buf(4, WB, NI, dtype=BF16), buf(NCH, 2, NI, WB),
            buf(NI, NI, dtype=BF16), buf(NI, NI, dtype=BF16), buf(NI, NI, dtype=BF16), buf(NI, NI, dtype=BF16),
            buf(8 * WB, NI, dtype=BF16),
            buf(NI, CW, dtype=BF16), buf(NI, CW, dtype=BF16), buf(NI, CW, dtype=BF16), buf(NI, CW, dtype=BF16),
            buf(NI, CW, dtype=BF16), buf(NCH, 2, 4, WB, CW),
            buf(NCH, 2, UP, CW), buf(NCH, 2, DN, CW), buf(NCH, 4, XR, CW), buf(2, NCH, UP, CW), buf(2, NCH, DN, CW),
            buf(NCH, 2, DN, CW), buf(NCH, 2, UP, CW),
            buf(NCH, XU, CW), buf(NCH, XD, CW), buf(NCH, RA, CW), buf(NCH, XR, CW), buf(NCH, XR, CW),
            buf(WB, a_gg.shape[2]), buf(2 * NCH, WB, WB), pltpu.SMEM((2 * NCH,), jnp.int32),
            dma((11,)), dma((7,)), dma((NCH,)), dma, dma((NCH,)), dma((14,)), dma((NCH, 14)),
        ],
        compiler_params=pltpu.CompilerParams(
            collective_id=0, has_side_effects=True, vmem_limit_bytes=52 * 2**20),
    )(
        fixed(interface_block[0, 0]), fixed(panel_order), fixed(lower_inverse[0, 0]), fixed(upper_inverse[0, 0]),
        fixed(left_coupling[0, 0].reshape(4, WB, NI)), fixed(right_pieces[0]), fixed(a_gg[0]))
    return schur[None]


def solution(mesh):
    return jax.shard_map(
        per_device,
        mesh=mesh,
        in_specs=(
            P("row", "col", None, None),
            P("row", "col", None, None),
            P("row", "col", None, None),
            P("col", None, "row"),
            P("row", "col", None),
            P("row", "col", None),
            P(),
        ),
        out_specs=P("row", "col", None),
        check_vma=False,
    )
```

```python
import functools

import jax
import jax.numpy as jnp
from jax import lax
from jax.experimental import pallas as pl
from jax.experimental.pallas import tpu as pltpu
from jax.sharding import PartitionSpec as P

MESH = pl.DeviceIdType.MESH
F32, BF16 = jnp.float32, jnp.bfloat16

NI = 1024
WB = 128
CW = 2 * WB
NCH = 8
TB = 256

UP, DN = 40, 32
XU, XD = 24, 32
RA = UP + DN
XR = XU + XD
A_UP, A_DN, A_ALL = pl.ds(0, UP), pl.ds(UP, DN), pl.ds(0, RA)
X_UP, X_DN, X_ALL = pl.ds(RA, XU), pl.ds(RA + XU, XD), pl.ds(RA, XR)

CHUNKS = ((0, 0), (-1, 0), (1, 0), (0, 1), (2, 0), (-1, 1), (1, 1), (2, 1))

LEFT_ORDER = tuple((dz, dx) for dz in (2, 1, 3, 0) for dx in (0, 1))

RING, RINGED = 4, (0, 1, 3, 4, 5, 6)
LONE = (2, 7, 8, 9, 10, 11, 12, 13)


def coords():
    r, c = lax.axis_index("row"), lax.axis_index("col")
    return r // 4, (r // 2) % 2, r % 2, c // 4, c % 4


def device(y, xl, core, xh, z):
    return (y * 4 + xl * 2 + core, xh * 4 + z)


def split(x):
    hi = x.astype(BF16)
    return hi, (x - hi.astype(F32)).astype(BF16)


def main_kernel(
    ids, order, low_hbm, upp_hbm, left_hbm, piece_hbm, base_hbm, out,
    low32, upp32, left_v, panel, low_hi, low_lo, upp_hi, upp_lo, left_d,
    p_hi, p_lo, h_hi, h_lo, solved, part,
    rp2, rq2, rx, up1, dn3, dn1, up3, rxp2, rxq2, fx2, fx1, fx3, base, total, origin,
    loc_sem, ag_s, ag_r, par_s, par_r, rs_s, rs_r, ring_r,
):
    y, xl, core, xh, z = coords()
    partner = device(y, xl, 1 - core, xh, z)
    across = device(y, 1 - xl, core, xh, z)
    ahead = device((y + 1 + 2 * core) % 4, xl, core, xh, z)
    behind = device((y + 3 + 2 * core) % 4, xl, core, xh, z)
    zp = device(y, xl, core, xh, (z + 1) % 4)
    zm = device(y, xl, core, xh, (z + 3) % 4)
    far = device(y, xl, core, 1 - xh, z)

    own = pltpu.make_async_copy(piece_hbm, panel.at[0, 0], loc_sem.at[0])
    own.start()
    loads = []
    for b in range(4):
        rows = pl.ds(b * TB, TB)
        cols = pl.ds(0, (b + 1) * TB)
        loads.append(pltpu.make_async_copy(low_hbm.at[rows, cols], low32.at[rows, cols], loc_sem.at[1 + b]))
    for b in range(4):
        rows = pl.ds(b * TB, TB)
        cols = pl.ds(b * TB, NI - b * TB)
        loads.append(pltpu.make_async_copy(upp_hbm.at[rows, cols], upp32.at[rows, cols], loc_sem.at[5 + b]))
    left_load = pltpu.make_async_copy(left_hbm, left_v, loc_sem.at[9])
    for copy in loads:
        copy.start()
    left_load.start()
    base_load = pltpu.make_async_copy(base_hbm, base, loc_sem.at[10])
    base_load.start()

    barrier = pltpu.get_barrier_semaphore()
    for peer in (partner, across, ahead, behind, zp, zm, far):
        pl.semaphore_signal(barrier, inc=1, device_id=peer, device_id_type=MESH)
    pl.semaphore_wait(barrier, 7)

    def link(n, src, dst, peer):
        return pltpu.make_async_remote_copy(
            src_ref=panel.at[src, 0], dst_ref=panel.at[dst, 0], send_sem=ag_s.at[min(n, 1)],
            recv_sem=ag_r.at[dst], device_id=peer, device_id_type=MESH)

    links = {
        1: link(0, 0, 1, ahead), 2: link(1, 0, 2, behind), 3: link(2, 0, 3, across), 4: link(3, 1, 4, ahead),
        5: link(4, 3, 5, ahead), 6: link(5, 3, 6, behind), 7: link(6, 6, 7, behind)}

    def share(i, at=None):
        return pltpu.make_async_remote_copy(
            src_ref=panel.at[i, 0], dst_ref=panel.at[i, 1], send_sem=par_s,
            recv_sem=par_r.at[i if at is None else at], device_id=partner, device_id_type=MESH)

    own.wait()
    share(0).start()
    links[1].start()
    links[3].start()

    strip = 64
    for b in range(4):
        loads[b].wait()

        @pl.loop(0, TB // strip)
        def _(s, b=b):
            rows = pl.ds(pl.multiple_of(b * TB + s * strip, strip), strip)
            cols = pl.ds(0, (b + 1) * TB)
            low_hi[rows, cols], low_lo[rows, cols] = split(low32[rows, cols])
    for b in range(4):
        loads[4 + b].wait()

        @pl.loop(0, TB // strip)
        def _(s, b=b):
            rows = pl.ds(pl.multiple_of(b * TB + s * strip, strip), strip)
            cols = pl.ds(b * TB, NI - b * TB)
            upp_hi[rows, cols], upp_lo[rows, cols] = split(upp32[rows, cols])

    left_load.wait()
    for n, (dz, dx) in enumerate(LEFT_ORDER):
        block = ((xh + dx) % 2) * 4 + (z + dz) % 4
        place = jnp.int32(0)
        touched = jnp.int32(0)
        for k in range(4):
            hit = ids[k] == block
            place = jnp.where(hit, k, place)
            touched = jnp.where(hit, 1, touched)
        left_d[n * WB:(n + 1) * WB] = jnp.where(touched > 0, left_v[place], jnp.zeros((WB, NI), BF16))

    def reduce_copies(i, at=None):
        at = i if at is None else at

        def send(n, src, dst, peer):
            slot = at % RING if n in RINGED else at
            return pltpu.make_async_remote_copy(
                src_ref=src, dst_ref=dst.at[i], send_sem=rs_s.at[n], recv_sem=(ring_r if n in RINGED else rs_r).at[slot, (RINGED if n in RINGED else LONE).index(n)],
                device_id=peer, device_id_type=MESH)

        both = slice(None)
        return {
            0: lambda: send(0, part.at[i, both, 2, A_UP], rp2, zp),
            1: lambda: send(1, part.at[i, both, 2, A_DN], rq2, zm),
            2: lambda: send(2, part.at[i, 1, both, X_ALL], rx, far),
            3: lambda: send(3, part.at[i, 1, 1, A_UP], up1.at[1], zp),
            4: lambda: send(4, part.at[i, 1, 3, A_DN], dn3.at[1], zm),
            10: lambda: send(10, part.at[i, 0, 1, A_UP], up1.at[0], zp),
            11: lambda: send(11, part.at[i, 0, 3, A_DN], dn3.at[0], zm),
            12: lambda: send(12, part.at[i, both, 1, A_DN], dn1, zp),
            13: lambda: send(13, part.at[i, both, 3, A_UP], up3, zm),
            5: lambda: send(5, part.at[i, 0, 2, X_UP], rxp2, zp),
            6: lambda: send(6, part.at[i, 0, 2, X_DN], rxq2, zm),
            7: lambda: send(7, part.at[i, 1, 0, A_ALL], fx2, far),
            8: lambda: send(8, part.at[i, 0, 1, X_ALL], fx1, zp),
            9: lambda: send(9, part.at[i, 0, 3, X_ALL], fx3, zm),
        }

    def start(i, *which):
        copies = reduce_copies(i)
        for n in which:
            copies[n]().start()

    def arrive(i, *which):
        copies = reduce_copies(i)
        for n in which:
            copies[n]().wait_recv()

    def multiply(i):
        for h in range(2):
            @pl.loop(0, 8)
            def _(s, h=h):
                rows = pl.ds(pl.multiple_of(s * WB, WB), WB)
                cols = pl.ds(h * WB, WB)
                p_hi[rows, cols], p_lo[rows, cols] = split(panel[i, h, rows, :])

        def dot(a, b):
            return jnp.dot(a, b, preferred_element_type=F32)

        for b in range(4):
            rows, cols = pl.ds(b * TB, TB), pl.ds(0, (b + 1) * TB)
            a_hi = low_hi[rows, cols]
            both = dot(jnp.concatenate([a_hi, low_lo[rows, cols]], axis=0), p_hi[cols])
            half = both[:TB] + both[TB:] + dot(a_hi, p_lo[cols])
            h_hi[rows, :], h_lo[rows, :] = split(half)
        for b in range(4):
            rows, cols = pl.ds(b * TB, TB), pl.ds(b * TB, NI - b * TB)
            a_hi = upp_hi[rows, cols]
            both = dot(jnp.concatenate([a_hi, upp_lo[rows, cols]], axis=0), h_hi[cols])
            full = both[:TB] + both[TB:] + dot(a_hi, h_lo[cols])
            solved[rows, :] = full.astype(BF16)
        for first_n in (0, 4):
            blocks = dot(left_d[first_n * WB:(first_n + 4) * WB], solved[...]).reshape(4, WB, CW)
            for n in range(4):
                dz, dx = LEFT_ORDER[first_n + n]
                part[i, dx, dz] = blocks[n]
        start(i, 0, 1, 12, 13, 2)

    def first(i):
        arrive(i, 0)
        part[i, :, 1, A_UP] += rp2[i]
        start(i, 3, 10)
        arrive(i, 1)
        part[i, :, 3, A_DN] += rq2[i]
        start(i, 4, 11)

    def second(i):
        arrive(i, 12, 13, 3, 4)
        part[i, 1, 0, A_UP] += up1[1, i] + up3[i, 1]
        part[i, 1, 0, A_DN] += dn1[i, 1] + dn3[1, i]
        start(i, 7)

    def cross(i):
        arrive(i, 2)
        part[i, 0, :, X_ALL] += rx[i]
        start(i, 5, 6)

    def along(i):
        arrive(i, 5)
        part[i, 0, 1, X_UP] += rxp2[i]
        start(i, 8)
        arrive(i, 6)
        part[i, 0, 3, X_DN] += rxq2[i]
        start(i, 9)

    def finish(i):
        arrive(i, 10, 11, 7)
        for rows, others in (
            (A_UP, up1[0, i] + up3[i, 0] + fx2[i, 0:UP]),
            (A_DN, dn1[i, 0] + dn3[0, i] + fx2[i, UP:RA]),
        ):
            summed = part[i, 0, 0, rows] + others
            for h in range(2):
                total[2 * i + h, rows] = summed[:, h * WB:(h + 1) * WB]
        arrive(i, 8, 9)
        rows = part[i, 0, 0, X_ALL] + (fx1[i] + fx3[i])
        for h in range(2):
            total[2 * i + h, X_ALL] = rows[:, h * WB:(h + 1) * WB]

    def pass_on(a, *then):
        links[a].wait_recv()
        share(a).start()
        for n in then:
            links[n].start()

    @pl.loop(0, NCH)
    def _(step):
        @pl.when(step == 1)
        def _():
            pass_on(1)
            first(0)

        @pl.when(step == 2)
        def _():
            links[4].start()
            pass_on(2)
            pass_on(3, 5, 6)
            first(1)

        @pl.when(step == 4)
        def _():
            pass_on(4)
            first(3)
            pass_on(6, 7)

        @pl.when(step == 5)
        def _():
            pass_on(5)
            first(4)

        @pl.when(step == 6)
        def _():
            pass_on(7)

        share(step).wait_recv()
        multiply(step)

        @pl.when(step == 0)
        def _():
            links[1].wait_send()
            links[2].start()

        @pl.when((step == 3) | (step >= 6))
        def _():
            first(step - 1)

        for lag, stage in ((2, cross), (2, second), (3, along), (5, finish)):
            @pl.when(step >= lag)
            def _(lag=lag, stage=stage):
                stage(step - lag)

    base_load.wait()
    places = []
    for dy, dx in CHUNKS:
        for h in range(2):
            holder = (core + h) % 2
            places.append(order[((y + 4 + dy * (1 - 2 * holder)) % 4) * 4 + ((xl + dx) % 2) * 2 + holder])
    for p in range(2 * NCH):
        found = jnp.int32(0)
        for t in range(2 * NCH):
            found = jnp.where(places[t] == p, t, found)
        origin[p] = found

    for i, stage in (
        (6, cross), (7, first), (7, cross), (6, second), (5, along), (6, along), (7, second), (7, along),
        (3, finish), (4, finish), (5, finish), (6, finish), (7, finish),
    ):
        stage(i)

    for p in range(2 * NCH):
        cols = slice(p * WB, (p + 1) * WB)
        out[:, cols] = base[:, cols] - total[origin[p]]

    six = panel.at[pl.ds(0, 6), 0]
    others = pltpu.make_async_remote_copy(
        src_ref=six, dst_ref=six, send_sem=ag_s.at[1], recv_sem=ag_r.at[0], device_id=ahead, device_id_type=MESH)
    others.wait_send()
    every = slice(None)
    share(every, 0).wait_send()
    for copy in reduce_copies(every, 0).values():
        copy().wait_send()


def per_device(lower_inverse, upper_inverse, left_coupling, right_pieces, interface_block, a_gg, panel_order):
    vmem = pl.BlockSpec(memory_space=pltpu.VMEM)
    smem = pl.BlockSpec(memory_space=pltpu.SMEM)
    hbm = pl.BlockSpec(memory_space=pltpu.HBM)

    def buf(*shape, dtype=F32):
        return pltpu.VMEM(shape, dtype)

    def fixed(x):
        return pltpu.with_memory_space_constraint(x, pltpu.HBM)

    dma = pltpu.SemaphoreType.DMA
    schur = pl.pallas_call(
        main_kernel,
        name="assemble",
        out_shape=jax.ShapeDtypeStruct(a_gg.shape[1:], F32),
        in_specs=[smem, smem, hbm, hbm, hbm, hbm, hbm],
        out_specs=vmem,
        scratch_shapes=[
            buf(NI, NI), buf(NI, NI), buf(4, WB, NI, dtype=BF16), buf(NCH, 2, NI, WB),
            buf(NI, NI, dtype=BF16), buf(NI, NI, dtype=BF16), buf(NI, NI, dtype=BF16), buf(NI, NI, dtype=BF16),
            buf(8 * WB, NI, dtype=BF16),
            buf(NI, CW, dtype=BF16), buf(NI, CW, dtype=BF16), buf(NI, CW, dtype=BF16), buf(NI, CW, dtype=BF16),
            buf(NI, CW, dtype=BF16), buf(NCH, 2, 4, WB, CW),
            buf(NCH, 2, UP, CW), buf(NCH, 2, DN, CW), buf(NCH, 4, XR, CW), buf(2, NCH, UP, CW), buf(2, NCH, DN, CW),
            buf(NCH, 2, DN, CW), buf(NCH, 2, UP, CW),
            buf(NCH, XU, CW), buf(NCH, XD, CW), buf(NCH, RA, CW), buf(NCH, XR, CW), buf(NCH, XR, CW),
            buf(WB, a_gg.shape[2]), buf(2 * NCH, WB, WB), pltpu.SMEM((2 * NCH,), jnp.int32),
            dma((11,)), dma((2,)), dma((NCH,)), dma, dma((NCH,)), dma((14,)), dma((NCH, len(LONE))), dma((RING, len(RINGED))),
        ],
        compiler_params=pltpu.CompilerParams(
            collective_id=0, has_side_effects=True, vmem_limit_bytes=52 * 2**20),
    )(
        fixed(interface_block[0, 0]), fixed(panel_order), fixed(lower_inverse[0, 0]), fixed(upper_inverse[0, 0]),
        fixed(left_coupling[0, 0].reshape(4, WB, NI)), fixed(right_pieces[0]), fixed(a_gg[0]))
    return schur[None]


def solution(mesh):
    return jax.shard_map(
        per_device,
        mesh=mesh,
        in_specs=(
            P("row", "col", None, None),
            P("row", "col", None, None),
            P("row", "col", None, None),
            P("col", None, "row"),
            P("row", "col", None),
            P("row", "col", None),
            P(),
        ),
        out_specs=P("row", "col", None),
        check_vma=False,
    )
```

```python
import functools

import jax
import jax.numpy as jnp
from jax import lax
from jax.experimental import pallas as pl
from jax.experimental.pallas import tpu as pltpu
from jax.sharding import PartitionSpec as P

MESH = pl.DeviceIdType.MESH
F32, BF16 = jnp.float32, jnp.bfloat16

NI = 1024
WB = 128
CW = 2 * WB
NCH = 8
TB = 256

UP, DN = 40, 32
XU, XD = 24, 32
RA = UP + DN
XR = XU + XD
A_UP, A_DN, A_ALL = pl.ds(0, UP), pl.ds(UP, DN), pl.ds(0, RA)
X_UP, X_DN, X_ALL = pl.ds(RA, XU), pl.ds(RA + XU, XD), pl.ds(RA, XR)

CHUNKS = ((0, 0), (-1, 0), (1, 0), (0, 1), (2, 0), (-1, 1), (1, 1), (2, 1))

LEFT_ORDER = tuple((dz, dx) for dz in (2, 1, 3, 0) for dx in (0, 1))

RING, RINGED = 4, (0, 1, 3, 4, 5, 6)
LONE = (2, 7, 8, 9, 10, 11, 12, 13)


def coords():
    r, c = lax.axis_index("row"), lax.axis_index("col")
    return r // 4, (r // 2) % 2, r % 2, c // 4, c % 4


def device(y, xl, core, xh, z):
    return (y * 4 + xl * 2 + core, xh * 4 + z)


def split(x):
    hi = x.astype(BF16)
    return hi, (x - hi.astype(F32)).astype(BF16)


def main_kernel(
    ids, order, low_hbm, upp_hbm, left_hbm, piece_hbm, base_hbm, out,
    low32, upp32, left_v, panel, low_hi, low_lo, upp_hi, upp_lo, left_d,
    p_hi, p_lo, h_hi, h_lo, solved, part,
    rp2, rq2, rx, up1, dn3, dn1, up3, rxp2, rxq2, fx2, fx1, fx3, base, total, origin,
    loc_sem, ag_s, ag_r, par_s, par_r, rs_s, rs_r, ring_r,
):
    y, xl, core, xh, z = coords()
    partner = device(y, xl, 1 - core, xh, z)
    across = device(y, 1 - xl, core, xh, z)
    ahead = device((y + 1 + 2 * core) % 4, xl, core, xh, z)
    behind = device((y + 3 + 2 * core) % 4, xl, core, xh, z)
    zp = device(y, xl, core, xh, (z + 1) % 4)
    zm = device(y, xl, core, xh, (z + 3) % 4)
    far = device(y, xl, core, 1 - xh, z)

    own = pltpu.make_async_copy(piece_hbm, panel.at[0, 0], loc_sem.at[0])
    own.start()
    loads = []
    for b in range(4):
        rows = pl.ds(b * TB, TB)
        cols = pl.ds(0, (b + 1) * TB)
        loads.append(pltpu.make_async_copy(low_hbm.at[rows, cols], low32.at[rows, cols], loc_sem.at[1 + b]))
    for b in range(4):
        rows = pl.ds(b * TB, TB)
        cols = pl.ds(b * TB, NI - b * TB)
        loads.append(pltpu.make_async_copy(upp_hbm.at[rows, cols], upp32.at[rows, cols], loc_sem.at[5 + b]))
    left_load = pltpu.make_async_copy(left_hbm, left_v, loc_sem.at[9])
    for copy in loads:
        copy.start()
    left_load.start()
    base_load = pltpu.make_async_copy(base_hbm, base, loc_sem.at[10])
    base_load.start()

    barrier = pltpu.get_barrier_semaphore()
    for peer in (partner, across, ahead, behind, zp, zm, far):
        pl.semaphore_signal(barrier, inc=1, device_id=peer, device_id_type=MESH)
    pl.semaphore_wait(barrier, 7)

    def link(n, src, dst, peer):
        return pltpu.make_async_remote_copy(
            src_ref=panel.at[src, 0], dst_ref=panel.at[dst, 0], send_sem=ag_s.at[min(n, 1)],
            recv_sem=ag_r.at[dst], device_id=peer, device_id_type=MESH)

    links = {
        1: link(0, 0, 1, ahead), 2: link(1, 0, 2, behind), 3: link(2, 0, 3, across), 4: link(3, 1, 4, ahead),
        5: link(4, 3, 5, ahead), 6: link(5, 3, 6, behind), 7: link(6, 6, 7, behind)}

    def share(i, at=None):
        return pltpu.make_async_remote_copy(
            src_ref=panel.at[i, 0], dst_ref=panel.at[i, 1], send_sem=par_s,
            recv_sem=par_r.at[i if at is None else at], device_id=partner, device_id_type=MESH)

    own.wait()
    share(0).start()
    links[1].start()
    links[3].start()

    strip = 64
    for b in range(4):
        loads[b].wait()

        @pl.loop(0, TB // strip)
        def _(s, b=b):
            rows = pl.ds(pl.multiple_of(b * TB + s * strip, strip), strip)
            cols = pl.ds(0, (b + 1) * TB)
            low_hi[rows, cols], low_lo[rows, cols] = split(low32[rows, cols])
    for b in range(4):
        loads[4 + b].wait()

        @pl.loop(0, TB // strip)
        def _(s, b=b):
            rows = pl.ds(pl.multiple_of(b * TB + s * strip, strip), strip)
            cols = pl.ds(b * TB, NI - b * TB)
            upp_hi[rows, cols], upp_lo[rows, cols] = split(upp32[rows, cols])

    left_load.wait()
    for n, (dz, dx) in enumerate(LEFT_ORDER):
        block = ((xh + dx) % 2) * 4 + (z + dz) % 4
        place = jnp.int32(0)
        touched = jnp.int32(0)
        for k in range(4):
            hit = ids[k] == block
            place = jnp.where(hit, k, place)
            touched = jnp.where(hit, 1, touched)
        left_d[n * WB:(n + 1) * WB] = jnp.where(touched > 0, left_v[place], jnp.zeros((WB, NI), BF16))

    def reduce_copies(i, at=None):
        at = i if at is None else at

        def send(n, src, dst, peer):
            slot = at % RING if n in RINGED else at
            return pltpu.make_async_remote_copy(
                src_ref=src, dst_ref=dst.at[i], send_sem=rs_s.at[n], recv_sem=(ring_r if n in RINGED else rs_r).at[slot, (RINGED if n in RINGED else LONE).index(n)],
                device_id=peer, device_id_type=MESH)

        both = slice(None)
        return {
            0: lambda: send(0, part.at[i, both, 2, A_UP], rp2, zp),
            1: lambda: send(1, part.at[i, both, 2, A_DN], rq2, zm),
            2: lambda: send(2, part.at[i, 1, both, X_ALL], rx, far),
            3: lambda: send(3, part.at[i, 1, 1, A_UP], up1.at[1], zp),
            4: lambda: send(4, part.at[i, 1, 3, A_DN], dn3.at[1], zm),
            10: lambda: send(10, part.at[i, 0, 1, A_UP], up1.at[0], zp),
            11: lambda: send(11, part.at[i, 0, 3, A_DN], dn3.at[0], zm),
            12: lambda: send(12, part.at[i, both, 1, A_DN], dn1, zp),
            13: lambda: send(13, part.at[i, both, 3, A_UP], up3, zm),
            5: lambda: send(5, part.at[i, 0, 2, X_UP], rxp2, zp),
            6: lambda: send(6, part.at[i, 0, 2, X_DN], rxq2, zm),
            7: lambda: send(7, part.at[i, 1, 0, A_ALL], fx2, far),
            8: lambda: send(8, part.at[i, 0, 1, X_ALL], fx1, zp),
            9: lambda: send(9, part.at[i, 0, 3, X_ALL], fx3, zm),
        }

    def start(i, *which):
        copies = reduce_copies(i)
        for n in which:
            copies[n]().start()

    def arrive(i, *which):
        copies = reduce_copies(i)
        for n in which:
            copies[n]().wait_recv()

    def multiply(i):
        for h in range(2):
            @pl.loop(0, 8)
            def _(s, h=h):
                rows = pl.ds(pl.multiple_of(s * WB, WB), WB)
                cols = pl.ds(h * WB, WB)
                p_hi[rows, cols], p_lo[rows, cols] = split(panel[i, h, rows, :])

        def dot(a, b):
            return jnp.dot(a, b, preferred_element_type=F32)

        for b in range(4):
            rows, cols = pl.ds(b * TB, TB), pl.ds(0, (b + 1) * TB)
            a_hi = low_hi[rows, cols]
            both = dot(jnp.concatenate([a_hi, low_lo[rows, cols]], axis=0), p_hi[cols])
            half = both[:TB] + both[TB:] + dot(a_hi, p_lo[cols])
            h_hi[rows, :], h_lo[rows, :] = split(half)
        for b in range(4):
            rows, cols = pl.ds(b * TB, TB), pl.ds(b * TB, NI - b * TB)
            a_hi = upp_hi[rows, cols]
            both = dot(jnp.concatenate([a_hi, upp_lo[rows, cols]], axis=0), h_hi[cols])
            full = both[:TB] + both[TB:] + dot(a_hi, h_lo[cols])
            solved[rows, :] = full.astype(BF16)
        for first_n in (0, 4):
            blocks = dot(left_d[first_n * WB:(first_n + 4) * WB], solved[...]).reshape(4, WB, CW)
            for n in range(4):
                dz, dx = LEFT_ORDER[first_n + n]
                part[i, dx, dz] = blocks[n]
        start(i, 0, 1, 12, 13, 2)

    def first(i):
        arrive(i, 0)
        part[i, :, 1, A_UP] += rp2[i]
        start(i, 3, 10)
        arrive(i, 1)
        part[i, :, 3, A_DN] += rq2[i]
        start(i, 4, 11)

    def second(i):
        arrive(i, 12, 13, 3, 4)
        part[i, 1, 0, A_UP] += up1[1, i] + up3[i, 1]
        part[i, 1, 0, A_DN] += dn1[i, 1] + dn3[1, i]
        start(i, 7)

    def cross(i):
        arrive(i, 2)
        part[i, 0, :, X_ALL] += rx[i]
        start(i, 5, 6)

    def along(i):
        arrive(i, 5)
        part[i, 0, 1, X_UP] += rxp2[i]
        start(i, 8)
        arrive(i, 6)
        part[i, 0, 3, X_DN] += rxq2[i]
        start(i, 9)

    def finish(i):
        arrive(i, 10, 11, 7)
        for rows, others in (
            (A_UP, up1[0, i] + up3[i, 0] + fx2[i, 0:UP]),
            (A_DN, dn1[i, 0] + dn3[0, i] + fx2[i, UP:RA]),
        ):
            summed = part[i, 0, 0, rows] + others
            for h in range(2):
                total[2 * i + h, rows] = summed[:, h * WB:(h + 1) * WB]
        arrive(i, 8, 9)
        rows = part[i, 0, 0, X_ALL] + (fx1[i] + fx3[i])
        for h in range(2):
            total[2 * i + h, X_ALL] = rows[:, h * WB:(h + 1) * WB]

    def pass_on(a, *then):
        links[a].wait_recv()
        share(a).start()
        for n in then:
            links[n].start()

    @pl.loop(0, NCH)
    def _(step):
        @pl.when(step == 1)
        def _():
            pass_on(1)
            first(0)

        @pl.when(step == 2)
        def _():
            links[4].start()
            pass_on(2)
            pass_on(3, 5, 6)
            first(1)

        @pl.when(step == 4)
        def _():
            pass_on(4)
            first(3)
            pass_on(6, 7)

        @pl.when(step == 5)
        def _():
            first(4)

        share(step).wait_recv()
        multiply(step)

        @pl.when(step == 0)
        def _():
            links[1].wait_send()
            links[2].start()

        @pl.when(step == 4)
        def _():
            pass_on(5)

        @pl.when(step == 5)
        def _():
            pass_on(7)

        @pl.when((step == 3) | (step >= 6))
        def _():
            first(step - 1)

        for lag, stage in ((2, cross), (2, second), (3, along), (5, finish)):
            @pl.when(step >= lag)
            def _(lag=lag, stage=stage):
                stage(step - lag)

    base_load.wait()
    places = []
    for dy, dx in CHUNKS:
        for h in range(2):
            holder = (core + h) % 2
            places.append(order[((y + 4 + dy * (1 - 2 * holder)) % 4) * 4 + ((xl + dx) % 2) * 2 + holder])
    for p in range(2 * NCH):
        found = jnp.int32(0)
        for t in range(2 * NCH):
            found = jnp.where(places[t] == p, t, found)
        origin[p] = found

    for i, stage in (
        (6, cross), (7, first), (7, cross), (6, second), (5, along), (6, along), (7, second), (7, along),
        (3, finish), (4, finish), (5, finish), (6, finish), (7, finish),
    ):
        stage(i)

    for p in range(2 * NCH):
        cols = slice(p * WB, (p + 1) * WB)
        out[:, cols] = base[:, cols] - total[origin[p]]

    six = panel.at[pl.ds(0, 6), 0]
    others = pltpu.make_async_remote_copy(
        src_ref=six, dst_ref=six, send_sem=ag_s.at[1], recv_sem=ag_r.at[0], device_id=ahead, device_id_type=MESH)
    others.wait_send()
    every = slice(None)
    share(every, 0).wait_send()
    for copy in reduce_copies(every, 0).values():
        copy().wait_send()


def per_device(lower_inverse, upper_inverse, left_coupling, right_pieces, interface_block, a_gg, panel_order):
    vmem = pl.BlockSpec(memory_space=pltpu.VMEM)
    smem = pl.BlockSpec(memory_space=pltpu.SMEM)
    hbm = pl.BlockSpec(memory_space=pltpu.HBM)

    def buf(*shape, dtype=F32):
        return pltpu.VMEM(shape, dtype)

    def fixed(x):
        return pltpu.with_memory_space_constraint(x, pltpu.HBM)

    dma = pltpu.SemaphoreType.DMA
    schur = pl.pallas_call(
        main_kernel,
        name="assemble",
        out_shape=jax.ShapeDtypeStruct(a_gg.shape[1:], F32),
        in_specs=[smem, smem, hbm, hbm, hbm, hbm, hbm],
        out_specs=vmem,
        scratch_shapes=[
            buf(NI, NI), buf(NI, NI), buf(4, WB, NI, dtype=BF16), buf(NCH, 2, NI, WB),
            buf(NI, NI, dtype=BF16), buf(NI, NI, dtype=BF16), buf(NI, NI, dtype=BF16), buf(NI, NI, dtype=BF16),
            buf(8 * WB, NI, dtype=BF16),
            buf(NI, CW, dtype=BF16), buf(NI, CW, dtype=BF16), buf(NI, CW, dtype=BF16), buf(NI, CW, dtype=BF16),
            buf(NI, CW, dtype=BF16), buf(NCH, 2, 4, WB, CW),
            buf(NCH, 2, UP, CW), buf(NCH, 2, DN, CW), buf(NCH, 4, XR, CW), buf(2, NCH, UP, CW), buf(2, NCH, DN, CW),
            buf(NCH, 2, DN, CW), buf(NCH, 2, UP, CW),
            buf(NCH, XU, CW), buf(NCH, XD, CW), buf(NCH, RA, CW), buf(NCH, XR, CW), buf(NCH, XR, CW),
            buf(WB, a_gg.shape[2]), buf(2 * NCH, WB, WB), pltpu.SMEM((2 * NCH,), jnp.int32),
            dma((11,)), dma((2,)), dma((NCH,)), dma, dma((NCH,)), dma((14,)), dma((NCH, len(LONE))), dma((RING, len(RINGED))),
        ],
        compiler_params=pltpu.CompilerParams(
            collective_id=0, has_side_effects=True, vmem_limit_bytes=52 * 2**20),
    )(
        fixed(interface_block[0, 0]), fixed(panel_order), fixed(lower_inverse[0, 0]), fixed(upper_inverse[0, 0]),
        fixed(left_coupling[0, 0].reshape(4, WB, NI)), fixed(right_pieces[0]), fixed(a_gg[0]))
    return schur[None]


def solution(mesh):
    return jax.shard_map(
        per_device,
        mesh=mesh,
        in_specs=(
            P("row", "col", None, None),
            P("row", "col", None, None),
            P("row", "col", None, None),
            P("col", None, "row"),
            P("row", "col", None),
            P("row", "col", None),
            P(),
        ),
        out_specs=P("row", "col", None),
        check_vma=False,
    )
```

```python
import functools

import jax
import jax.numpy as jnp
from jax import lax
from jax.experimental import pallas as pl
from jax.experimental.pallas import tpu as pltpu
from jax.sharding import PartitionSpec as P

MESH = pl.DeviceIdType.MESH
F32, BF16 = jnp.float32, jnp.bfloat16

NI = 1024
WB = 128
CW = 2 * WB
NCH = 8
TB = 256

UP, DN = 40, 32
XU, XD = 24, 32
RA = UP + DN
XR = XU + XD
A_UP, A_DN, A_ALL = pl.ds(0, UP), pl.ds(UP, DN), pl.ds(0, RA)
X_UP, X_DN, X_ALL = pl.ds(RA, XU), pl.ds(RA + XU, XD), pl.ds(RA, XR)

CHUNKS = ((0, 0), (-1, 0), (1, 0), (0, 1), (2, 0), (-1, 1), (1, 1), (2, 1))

LEFT_ORDER = tuple((dz, dx) for dz in (2, 1, 3, 0) for dx in (0, 1))

RING, RINGED = 4, (0, 1, 3, 4, 5, 6)
LONE = (2, 7, 8, 9, 10, 11, 12, 13)


def coords():
    r, c = lax.axis_index("row"), lax.axis_index("col")
    return r // 4, (r // 2) % 2, r % 2, c // 4, c % 4


def device(y, xl, core, xh, z):
    return (y * 4 + xl * 2 + core, xh * 4 + z)


def split(x):
    hi = x.astype(BF16)
    return hi, (x - hi.astype(F32)).astype(BF16)


def main_kernel(
    ids, order, low_hbm, upp_hbm, left_hbm, piece_hbm, base_hbm, out,
    low32, upp32, left_v, panel, low_hi, low_lo, upp_hi, upp_lo, left_d,
    p_hi, p_lo, h_hi, h_lo, solved, part,
    rp2, rq2, rx, up1, dn3, dn1, up3, rxp2, rxq2, fx2, fx1, fx3, base, total, origin,
    loc_sem, ag_s, ag_r, par_s, par_r, rs_s, rs_r, ring_r,
):
    y, xl, core, xh, z = coords()
    partner = device(y, xl, 1 - core, xh, z)
    across = device(y, 1 - xl, core, xh, z)
    ahead = device((y + 1 + 2 * core) % 4, xl, core, xh, z)
    behind = device((y + 3 + 2 * core) % 4, xl, core, xh, z)
    zp = device(y, xl, core, xh, (z + 1) % 4)
    zm = device(y, xl, core, xh, (z + 3) % 4)
    far = device(y, xl, core, 1 - xh, z)

    own = pltpu.make_async_copy(piece_hbm, panel.at[0, 0], loc_sem.at[0])
    own.start()
    loads = []
    for b in range(4):
        rows = pl.ds(b * TB, TB)
        cols = pl.ds(0, (b + 1) * TB)
        loads.append(pltpu.make_async_copy(low_hbm.at[rows, cols], low32.at[rows, cols], loc_sem.at[1 + b]))
    for b in range(4):
        rows = pl.ds(b * TB, TB)
        cols = pl.ds(b * TB, NI - b * TB)
        loads.append(pltpu.make_async_copy(upp_hbm.at[rows, cols], upp32.at[rows, cols], loc_sem.at[5 + b]))
    left_load = pltpu.make_async_copy(left_hbm, left_v, loc_sem.at[9])
    for copy in loads:
        copy.start()
    left_load.start()
    base_load = pltpu.make_async_copy(base_hbm, base, loc_sem.at[10])
    base_load.start()

    barrier = pltpu.get_barrier_semaphore()
    for peer in (partner, across, ahead, behind, zp, zm, far):
        pl.semaphore_signal(barrier, inc=1, device_id=peer, device_id_type=MESH)
    pl.semaphore_wait(barrier, 7)

    def link(n, src, dst, peer):
        return pltpu.make_async_remote_copy(
            src_ref=panel.at[src, 0], dst_ref=panel.at[dst, 0], send_sem=ag_s.at[min(n, 1)],
            recv_sem=ag_r.at[dst], device_id=peer, device_id_type=MESH)

    links = {
        1: link(0, 0, 1, ahead), 2: link(1, 0, 2, behind), 3: link(2, 0, 3, across), 4: link(3, 1, 4, ahead),
        5: link(4, 3, 5, ahead), 6: link(5, 3, 6, behind), 7: link(6, 6, 7, behind)}

    def share(i, at=None):
        return pltpu.make_async_remote_copy(
            src_ref=panel.at[i, 0], dst_ref=panel.at[i, 1], send_sem=par_s,
            recv_sem=par_r.at[i if at is None else at], device_id=partner, device_id_type=MESH)

    own.wait()
    share(0).start()
    links[1].start()
    links[3].start()

    strip = 128
    for b in range(4):
        loads[b].wait()

        @pl.loop(0, TB // strip)
        def _(s, b=b):
            rows = pl.ds(pl.multiple_of(b * TB + s * strip, strip), strip)
            cols = pl.ds(0, (b + 1) * TB)
            low_hi[rows, cols], low_lo[rows, cols] = split(low32[rows, cols])
    for b in range(4):
        loads[4 + b].wait()

        @pl.loop(0, TB // strip)
        def _(s, b=b):
            rows = pl.ds(pl.multiple_of(b * TB + s * strip, strip), strip)
            cols = pl.ds(b * TB, NI - b * TB)
            upp_hi[rows, cols], upp_lo[rows, cols] = split(upp32[rows, cols])

    left_load.wait()
    for n, (dz, dx) in enumerate(LEFT_ORDER):
        block = ((xh + dx) % 2) * 4 + (z + dz) % 4
        place = jnp.int32(0)
        touched = jnp.int32(0)
        for k in range(4):
            hit = ids[k] == block
            place = jnp.where(hit, k, place)
            touched = jnp.where(hit, 1, touched)
        left_d[n * WB:(n + 1) * WB] = jnp.where(touched > 0, left_v[place], jnp.zeros((WB, NI), BF16))

    def reduce_copies(i, at=None):
        at = i if at is None else at

        def send(n, src, dst, peer):
            slot = at % RING if n in RINGED else at
            return pltpu.make_async_remote_copy(
                src_ref=src, dst_ref=dst.at[i], send_sem=rs_s.at[n], recv_sem=(ring_r if n in RINGED else rs_r).at[slot, (RINGED if n in RINGED else LONE).index(n)],
                device_id=peer, device_id_type=MESH)

        both = slice(None)
        return {
            0: lambda: send(0, part.at[i, both, 2, A_UP], rp2, zp),
            1: lambda: send(1, part.at[i, both, 2, A_DN], rq2, zm),
            2: lambda: send(2, part.at[i, 1, both, X_ALL], rx, far),
            3: lambda: send(3, part.at[i, 1, 1, A_UP], up1.at[1], zp),
            4: lambda: send(4, part.at[i, 1, 3, A_DN], dn3.at[1], zm),
            10: lambda: send(10, part.at[i, 0, 1, A_UP], up1.at[0], zp),
            11: lambda: send(11, part.at[i, 0, 3, A_DN], dn3.at[0], zm),
            12: lambda: send(12, part.at[i, both, 1, A_DN], dn1, zp),
            13: lambda: send(13, part.at[i, both, 3, A_UP], up3, zm),
            5: lambda: send(5, part.at[i, 0, 2, X_UP], rxp2, zp),
            6: lambda: send(6, part.at[i, 0, 2, X_DN], rxq2, zm),
            7: lambda: send(7, part.at[i, 1, 0, A_ALL], fx2, far),
            8: lambda: send(8, part.at[i, 0, 1, X_ALL], fx1, zp),
            9: lambda: send(9, part.at[i, 0, 3, X_ALL], fx3, zm),
        }

    def start(i, *which):
        copies = reduce_copies(i)
        for n in which:
            copies[n]().start()

    def arrive(i, *which):
        copies = reduce_copies(i)
        for n in which:
            copies[n]().wait_recv()

    def multiply(i):
        for h in range(2):
            @pl.loop(0, 4)
            def _(s, h=h):
                rows = pl.ds(pl.multiple_of(s * TB, TB), TB)
                cols = pl.ds(h * WB, WB)
                p_hi[rows, cols], p_lo[rows, cols] = split(panel[i, h, rows, :])

        def dot(a, b):
            return jnp.dot(a, b, preferred_element_type=F32)

        for b in range(4):
            rows, cols = pl.ds(b * TB, TB), pl.ds(0, (b + 1) * TB)
            a_hi = low_hi[rows, cols]
            both = dot(jnp.concatenate([a_hi, low_lo[rows, cols]], axis=0), p_hi[cols])
            half = both[:TB] + both[TB:] + dot(a_hi, p_lo[cols])
            h_hi[rows, :], h_lo[rows, :] = split(half)
        for b in range(4):
            rows, cols = pl.ds(b * TB, TB), pl.ds(b * TB, NI - b * TB)
            a_hi = upp_hi[rows, cols]
            both = dot(jnp.concatenate([a_hi, upp_lo[rows, cols]], axis=0), h_hi[cols])
            full = both[:TB] + both[TB:] + dot(a_hi, h_lo[cols])
            solved[rows, :] = full.astype(BF16)
        for first_n in (0, 4):
            blocks = dot(left_d[first_n * WB:(first_n + 4) * WB], solved[...]).reshape(4, WB, CW)
            for n in range(4):
                dz, dx = LEFT_ORDER[first_n + n]
                part[i, dx, dz] = blocks[n]
        start(i, 0, 1, 12, 13, 2)

    def first(i):
        arrive(i, 0)
        part[i, :, 1, A_UP] += rp2[i]
        start(i, 3, 10)
        arrive(i, 1)
        part[i, :, 3, A_DN] += rq2[i]
        start(i, 4, 11)

    def second(i):
        arrive(i, 12, 13, 3, 4)
        part[i, 1, 0, A_UP] += up1[1, i] + up3[i, 1]
        part[i, 1, 0, A_DN] += dn1[i, 1] + dn3[1, i]
        start(i, 7)

    def cross(i):
        arrive(i, 2)
        part[i, 0, :, X_ALL] += rx[i]
        start(i, 5, 6)

    def along(i):
        arrive(i, 5)
        part[i, 0, 1, X_UP] += rxp2[i]
        start(i, 8)
        arrive(i, 6)
        part[i, 0, 3, X_DN] += rxq2[i]
        start(i, 9)

    def finish(i):
        arrive(i, 10, 11, 7)
        for rows, others in (
            (A_UP, up1[0, i] + up3[i, 0] + fx2[i, 0:UP]),
            (A_DN, dn1[i, 0] + dn3[0, i] + fx2[i, UP:RA]),
        ):
            summed = part[i, 0, 0, rows] + others
            for h in range(2):
                total[2 * i + h, rows] = summed[:, h * WB:(h + 1) * WB]
        arrive(i, 8, 9)
        rows = part[i, 0, 0, X_ALL] + (fx1[i] + fx3[i])
        for h in range(2):
            total[2 * i + h, X_ALL] = rows[:, h * WB:(h + 1) * WB]

    def pass_on(a, *then):
        links[a].wait_recv()
        share(a).start()
        for n in then:
            links[n].start()

    @pl.loop(0, NCH)
    def _(step):
        @pl.when(step == 1)
        def _():
            pass_on(1)
            first(0)

        @pl.when(step == 2)
        def _():
            links[4].start()
            pass_on(2)
            pass_on(3, 5, 6)
            first(1)

        @pl.when(step == 4)
        def _():
            pass_on(4)
            first(3)
            pass_on(6, 7)

        @pl.when(step == 5)
        def _():
            first(4)

        share(step).wait_recv()
        multiply(step)

        @pl.when(step == 0)
        def _():
            links[1].wait_send()
            links[2].start()

        @pl.when(step == 4)
        def _():
            pass_on(5)

        @pl.when(step == 5)
        def _():
            pass_on(7)

        @pl.when((step == 3) | (step >= 6))
        def _():
            first(step - 1)

        for lag, stage in ((2, cross), (2, second), (3, along), (5, finish)):
            @pl.when(step >= lag)
            def _(lag=lag, stage=stage):
                stage(step - lag)

    base_load.wait()
    places = []
    for dy, dx in CHUNKS:
        for h in range(2):
            holder = (core + h) % 2
            places.append(order[((y + 4 + dy * (1 - 2 * holder)) % 4) * 4 + ((xl + dx) % 2) * 2 + holder])
    for p in range(2 * NCH):
        found = jnp.int32(0)
        for t in range(2 * NCH):
            found = jnp.where(places[t] == p, t, found)
        origin[p] = found

    for i, stage in (
        (6, cross), (7, first), (7, cross), (6, second), (5, along), (6, along), (7, second), (7, along),
        (3, finish), (4, finish), (5, finish), (6, finish), (7, finish),
    ):
        stage(i)

    for p in range(2 * NCH):
        cols = slice(p * WB, (p + 1) * WB)
        out[:, cols] = base[:, cols] - total[origin[p]]

    six = panel.at[pl.ds(0, 6), 0]
    others = pltpu.make_async_remote_copy(
        src_ref=six, dst_ref=six, send_sem=ag_s.at[1], recv_sem=ag_r.at[0], device_id=ahead, device_id_type=MESH)
    others.wait_send()
    every = slice(None)
    share(every, 0).wait_send()
    for copy in reduce_copies(every, 0).values():
        copy().wait_send()


def per_device(lower_inverse, upper_inverse, left_coupling, right_pieces, interface_block, a_gg, panel_order):
    vmem = pl.BlockSpec(memory_space=pltpu.VMEM)
    smem = pl.BlockSpec(memory_space=pltpu.SMEM)
    hbm = pl.BlockSpec(memory_space=pltpu.HBM)

    def buf(*shape, dtype=F32):
        return pltpu.VMEM(shape, dtype)

    def fixed(x):
        return pltpu.with_memory_space_constraint(x, pltpu.HBM)

    dma = pltpu.SemaphoreType.DMA
    schur = pl.pallas_call(
        main_kernel,
        name="assemble",
        out_shape=jax.ShapeDtypeStruct(a_gg.shape[1:], F32),
        in_specs=[smem, smem, hbm, hbm, hbm, hbm, hbm],
        out_specs=vmem,
        scratch_shapes=[
            buf(NI, NI), buf(NI, NI), buf(4, WB, NI, dtype=BF16), buf(NCH, 2, NI, WB),
            buf(NI, NI, dtype=BF16), buf(NI, NI, dtype=BF16), buf(NI, NI, dtype=BF16), buf(NI, NI, dtype=BF16),
            buf(8 * WB, NI, dtype=BF16),
            buf(NI, CW, dtype=BF16), buf(NI, CW, dtype=BF16), buf(NI, CW, dtype=BF16), buf(NI, CW, dtype=BF16),
            buf(NI, CW, dtype=BF16), buf(NCH, 2, 4, WB, CW),
            buf(NCH, 2, UP, CW), buf(NCH, 2, DN, CW), buf(NCH, 4, XR, CW), buf(2, NCH, UP, CW), buf(2, NCH, DN, CW),
            buf(NCH, 2, DN, CW), buf(NCH, 2, UP, CW),
            buf(NCH, XU, CW), buf(NCH, XD, CW), buf(NCH, RA, CW), buf(NCH, XR, CW), buf(NCH, XR, CW),
            buf(WB, a_gg.shape[2]), buf(2 * NCH, WB, WB), pltpu.SMEM((2 * NCH,), jnp.int32),
            dma((11,)), dma((2,)), dma((NCH,)), dma, dma((NCH,)), dma((14,)), dma((NCH, len(LONE))), dma((RING, len(RINGED))),
        ],
        compiler_params=pltpu.CompilerParams(
            collective_id=0, has_side_effects=True, vmem_limit_bytes=52 * 2**20),
    )(
        fixed(interface_block[0, 0]), fixed(panel_order), fixed(lower_inverse[0, 0]), fixed(upper_inverse[0, 0]),
        fixed(left_coupling[0, 0].reshape(4, WB, NI)), fixed(right_pieces[0]), fixed(a_gg[0]))
    return schur[None]


def solution(mesh):
    return jax.shard_map(
        per_device,
        mesh=mesh,
        in_specs=(
            P("row", "col", None, None),
            P("row", "col", None, None),
            P("row", "col", None, None),
            P("col", None, "row"),
            P("row", "col", None),
            P("row", "col", None),
            P(),
        ),
        out_specs=P("row", "col", None),
        check_vma=False,
    )
```
